256 devices in a mesh: segment: 4 (over x), amp: 64 (over y, z, core).
Axes of the slice: x: 4, y: 4, z: 8, core: 2. Of those that a mesh axis runs over, the one named last changes fastest.
Arguments:
- states: float32 [4, 16777216], P('segment', 'amp'), may hold values from -6 to 6
- gate_blocks: float32 [4, 3, 128, 128], P('segment'), may hold values from -1 to 1, as said below
- kraus_picks: int32 [4, 4, 3, 7], P('segment'), may hold values from 0 to 3
- block_targets: int32 [4, 3], replicated, may hold values from 0 to 1
Outputs:
- final_states: float32 [4, 16777216], P('segment', 'amp')
- log_weights: float32 [4, 4], P('segment')
The draws below stay inside these ranges and needn't reach their ends.
Inputs may be any that keep to these rules, and one draw needn't show every extreme that they name: Every block of gate_blocks is an orthogonal matrix, up to rounding.
All inputs are finite; a program needn't handle non-finite values.
Results may differ from the reference program's by a relative error of at most 0.0003.
Values sent between devices are 32-bit elements; how exact they have to be, the bound alone decides.
A program may use at most 64 MiB of HBM per device.

```python
import jax
import jax.numpy as jnp
from jax import lax

QB = 7
REG = 128
MIDC = 16
BLOCKS = 3
SECTIONS = 4
TRAJ = 4
GLOBALS = 64
AMPS = 16777216


def draw_gate_blocks(key, part):
    gaussian = jax.random.normal(key, (SECTIONS, BLOCKS, REG, REG), jnp.float32)
    q_factor, r_factor = jnp.linalg.qr(gaussian)
    return q_factor.astype(jnp.float32)


def place_ends(array, key, low, largest):
    place = [jax.random.randint(jax.random.fold_in(key, axis), (), 0, length) for axis, length in enumerate(array.shape)]
    main_axis = array.shape.index(max(array.shape))
    beside = place[:main_axis] + [(place[main_axis] + 1) % array.shape[main_axis]] + place[main_axis + 1:]
    return array.at[tuple(place)].set(low).at[tuple(beside)].set(largest)


def level_of(rng, extent, shards, smallest, largest):
    factor_of = 1.0
    for axis_at, shards_of in shards:
        heights = jax.random.uniform(jax.random.fold_in(jax.random.fold_in(rng, 6), axis_at), (shards_of,), jnp.float32, smallest / len(shards), largest / len(shards))
        factor_of = factor_of * jnp.repeat(jnp.exp(heights), extent[axis_at] // shards_of).reshape((-1,) + (1,) * (len(extent) - 1 - axis_at))
    return factor_of


def normal_values(own_key, extent, deviation, most, cuts=(), kind=jnp.bfloat16):
    gain = level_of(own_key, extent, cuts, -0.22, 0.18) if cuts else 1.0
    values = jax.random.normal(own_key, extent, jnp.float32) * deviation * gain
    return jnp.minimum(jnp.maximum(values, -most), most).astype(kind)


def setup_inputs(seed: int = 0) -> dict:
    arg_keys = jax.random.split(jax.random.key(seed), 5)
    states = normal_values(arg_keys[0], (TRAJ, AMPS), 1.0, 6.0, ((0, 4), (1, 64)), jnp.float32)
    gate_blocks = draw_gate_blocks(jax.random.fold_in(arg_keys[4], 71), 0)
    kraus_picks = place_ends(jax.random.randint(arg_keys[2], (TRAJ, SECTIONS, BLOCKS, QB), 0, 4), jax.random.fold_in(arg_keys[2], 1), 0, 3).astype(jnp.int32)
    block_targets = place_ends(jax.random.randint(arg_keys[3], (SECTIONS, BLOCKS), 0, 2), jax.random.fold_in(arg_keys[3], 1), 0, 1).astype(jnp.int32)
    return {"states": states, "gate_blocks": gate_blocks, "kraus_picks": kraus_picks, "block_targets": block_targets}


KEEP_FACTORS = (1.0, 0.9, 1.0, 0.97)
FLIP_FACTORS = (0.9, 1.0, 0.97, 1.0)

def noise_factors(kraus_rows):
    qubit_count = kraus_rows.shape[-1]
    register = 2 ** qubit_count
    positions = jnp.arange(register, dtype=jnp.int32)
    product = jnp.ones(kraus_rows.shape[:-1] + (register,), jnp.float32)
    for qubit_pos in range(qubit_count):
        bit_value = jnp.right_shift(positions, qubit_count - 1 - qubit_pos) & 1
        column = kraus_rows[..., qubit_pos:qubit_pos + 1]
        low_value = jnp.zeros(column.shape, jnp.float32)
        high_value = jnp.zeros(column.shape, jnp.float32)
        for option in range(4):
            picked = (column == option).astype(jnp.float32)
            low_value = low_value + picked * KEEP_FACTORS[option]
            high_value = high_value + picked * FLIP_FACTORS[option]
        product = product * jnp.where(bit_value == 1, high_value, low_value)
    return product

def apply_gate(amplitudes, matrix, factors, target):

    def on_low(values):
        mixed_rows = jnp.einsum('bghmk,ik->bghmi', values, matrix, precision=lax.Precision.HIGHEST)
        return mixed_rows * factors[:, None, None, None, :]

    def on_high(values):
        mixed_rows = jnp.einsum('bgjmk,ij->bgimk', values, matrix, precision=lax.Precision.HIGHEST)
        return mixed_rows * factors[:, None, :, None, None]
    return lax.cond(target == 0, on_low, on_high, amplitudes)

def swap_global(amplitudes):
    traj_all, global_count, register, middle, low_count = amplitudes.shape
    split_view = amplitudes.reshape(traj_all, global_count, global_count, register // global_count, middle, low_count)
    swapped = jnp.swapaxes(split_view, 1, 2)
    return swapped.reshape(traj_all, global_count, register, middle, low_count)

def reference(states, gate_blocks, kraus_picks, block_targets):
    register = gate_blocks.shape[-1]
    amplitudes = states.reshape(TRAJ, GLOBALS, register, MIDC, register)
    mean_sq = lax.optimization_barrier(jnp.mean(amplitudes * amplitudes, axis=(1, 2, 3, 4)))
    amplitudes = amplitudes / jnp.sqrt(mean_sq)[:, None, None, None, None]
    log_list = []
    for section in range(SECTIONS):
        for block_pos in range(BLOCKS):
            factors = noise_factors(kraus_picks[:, section, block_pos, :])
            amplitudes = apply_gate(amplitudes, gate_blocks[section, block_pos], factors, block_targets[section, block_pos])
        amplitudes = swap_global(amplitudes)
        mean_sq = lax.optimization_barrier(jnp.mean(amplitudes * amplitudes, axis=(1, 2, 3, 4)))
        log_list.append(jnp.log(mean_sq))
        amplitudes = amplitudes / jnp.sqrt(mean_sq)[:, None, None, None, None]
    return (amplitudes.reshape(TRAJ, AMPS), jnp.stack(log_list, axis=1))
```

```python
import functools

import jax
import jax.numpy as jnp
from jax import lax
from jax.experimental import pallas as pl
from jax.experimental.pallas import tpu as pltpu
from jax.sharding import PartitionSpec as P

KEEP_FACTORS = (1.0, 0.9, 1.0, 0.97)
FLIP_FACTORS = (0.9, 1.0, 0.97, 1.0)
QUBITS = 7
REG = 128
MID = 16
PEERS = 64
SECTIONS = 4
BLOCKS = 3
ROWS = 2048
MESH = pl.DeviceIdType.MESH
F32 = jnp.float32
BF16 = jnp.bfloat16


def split(x):
    hi = x.astype(BF16)
    lo = (x - hi.astype(F32)).astype(BF16)
    return hi, lo


def exact_dot(a, b):
    return jnp.dot(a, b, precision=lax.Precision.HIGHEST, preferred_element_type=F32)


def mix_rows(gate_cat, x):
    hi, lo = split(x)
    return jnp.dot(gate_cat, jnp.concatenate([hi, hi, lo], axis=0), preferred_element_type=F32)


def mix_lanes(x, gate_cat):
    hi, lo = split(x)
    return jnp.dot(jnp.concatenate([hi, hi, lo], axis=1), gate_cat, preferred_element_type=F32)


def rows_cat(gate):
    hi, lo = split(gate)
    return jnp.concatenate([hi, lo, hi], axis=1)


def lanes_cat(gate_t):
    hi, lo = split(gate_t)
    return jnp.concatenate([hi, lo, hi], axis=0)


def block_transpose(arrays):
    lane = lax.broadcasted_iota(jnp.int32, arrays[0].shape, 1)
    low_half = lane < 64
    even = (lane // 32) % 2 == 0
    stage = [None] * 4
    for a in range(2):
        moved = pltpu.roll(jnp.where(low_half, arrays[a + 2], arrays[a]), 64, 1)
        stage[a] = jnp.where(low_half, arrays[a], moved)
        stage[a + 2] = jnp.where(low_half, moved, arrays[a + 2])
    result = [None] * 4
    for a in (0, 2):
        result[a] = jnp.where(even, stage[a], pltpu.roll(stage[a + 1], 32, 1))
        result[a + 1] = jnp.where(even, pltpu.roll(stage[a], 96, 1), stage[a + 1])
    return result


def fold_squares(acc, x):
    sq = x * x
    return acc + jnp.sum(sq.reshape(sq.shape[0] // 8, 8, sq.shape[1]), axis=0)


def amp_of(m, j):
    return (m // 8) * 32 + (j // 2) * 16 + (m % 8) * 2 + j % 2


def scalar_pick(kind, table):
    return jnp.where(
        kind == 0,
        F32(table[0]),
        jnp.where(kind == 1, F32(table[1]), jnp.where(kind == 2, F32(table[2]), F32(table[3]))),
    )


def kernel(
    x_ref, gate_ref, kraus_ref, target_ref,
    y_ref, stats_ref,
    all_gates, send1, recv1, mid2, mid3, half2, recv2, send3, recv3, h_mats, l01_mat, l2_mat, l23_mat, sums_out, sums_in,
    gate_send, gate_recv, pair_send, pair_recv,
    send1_sem, recv1_sem, send2_sem, recv2_sem, send3_sem, recv3_sem, sums_send, sums_recv,
):
    seg = lax.axis_index("segment")
    me = lax.axis_index("amp")
    y_pos = me // 16
    j_me = (y_pos % 2) * 2 + me % 2
    m_me = (y_pos // 2) * 8 + (me % 16) // 2
    core = me % 2
    partner = me + 1 - 2 * core
    zero = jnp.zeros((8, REG), F32)

    def at(ref, index, rows):
        return ref.at[pl.ds(pl.multiple_of(index * rows, rows), rows)]

    barrier = pltpu.get_barrier_semaphore()

    def greet(k, carry):
        pl.semaphore_signal(barrier, inc=1, device_id=(seg, (me + k) % PEERS), device_id_type=MESH)
        return carry

    lax.fori_loop(1, PEERS, greet, 0)
    for k in range(1, SECTIONS):
        pl.semaphore_signal(barrier, inc=1, device_id=((seg + k) % SECTIONS, me), device_id_type=MESH)

    all_gates[seg] = gate_ref[...]

    pl.semaphore_wait(barrier, PEERS - 1 + SECTIONS - 1)

    my_half = pl.ds(pl.multiple_of(core * 64, 64), 64)
    other_half = pl.ds(pl.multiple_of((1 - core) * 64, 64), 64)

    def gate_copy(section, target_seg):
        return pltpu.make_async_remote_copy(
            gate_ref.at[:, my_half, :],
            all_gates.at[section, :, my_half, :],
            gate_send.at[target_seg],
            gate_recv.at[section],
            device_id=(target_seg, me),
            device_id_type=MESH,
        )

    def pair_copy(section):
        return pltpu.make_async_remote_copy(
            all_gates.at[section, :, my_half, :],
            all_gates.at[section, :, my_half, :],
            pair_send.at[section],
            pair_recv.at[section],
            device_id=(seg, partner),
            device_id_type=MESH,
        )

    def send_gates(section):
        @pl.when(seg == section)
        def _():
            for k in range(1, SECTIONS):
                gate_copy(section, (seg + k) % SECTIONS).start()

    def pass_gates(section):
        @pl.when(seg != section)
        def _():
            gate_copy(section, section).wait_recv()
            pair_copy(section).start()

    def end_gates(section):
        @pl.when(seg != section)
        def _():
            pltpu.make_async_copy(
                all_gates.at[section, :, other_half, :], all_gates.at[section, :, other_half, :], pair_recv.at[section]
            ).wait()

    row = lax.broadcasted_iota(jnp.int32, (REG, REG), 0)
    col = lax.broadcasted_iota(jnp.int32, (REG, REG), 1)
    identity = (row == col).astype(F32)
    to_split = (col == (row % 64) * 2 + row // 64).astype(F32)
    from_split = (row == (col % 64) * 2 + col // 64).astype(F32)

    def noise(section, block):
        product = jnp.ones((REG, REG), F32)
        for q in range(QUBITS):
            kind = kraus_ref[section, block, q]
            bit = lax.shift_right_logical(row, QUBITS - 1 - q) & 1
            product = product * jnp.where(bit == 1, scalar_pick(kind, FLIP_FACTORS), scalar_pick(kind, KEEP_FACTORS))
        return product

    def compose(section):
        low, high = identity, identity
        for block in range(BLOCKS):
            on_low = target_ref[section, block] == 0
            gate = all_gates[section, block]
            if block == 0:
                mixed = gate
            else:
                mixed = exact_dot(gate, jnp.where(on_low, low, high))
            mixed = noise(section, block) * mixed
            low, high = jnp.where(on_low, mixed, low), jnp.where(on_low, high, mixed)
        return low, high

    send_gates(0)
    send_gates(1)
    pass_gates(0)
    pass_gates(1)
    end_gates(0)
    low0, high0 = compose(0)
    h_mats[0] = rows_cat(high0)
    end_gates(1)
    low1, high1 = compose(1)
    h_mats[1] = rows_cat(exact_dot(high1, from_split))
    l01_mat[...] = jnp.concatenate([lanes_cat(low0.T), lanes_cat(exact_dot(low1, low0).T)], axis=1)

    width = 2

    def send_piece1(m, j):
        to = amp_of(m, j)

        @pl.when(to != me)
        def _():
            pltpu.make_async_remote_copy(
                at(send1, m * 4 + j, 32), at(recv1, me, 32), send1_sem, recv1_sem, device_id=(seg, to), device_id_type=MESH
            ).start()

    def send_chunk1(k):
        def one(n, carry):
            send_piece1((m_me + k * width + n // 4) % MID, (j_me + n) % 4)
            return carry

        lax.fori_loop(0, 4 * width, one, 0)

    def section0(k, sums):
        first, after = sums
        ms = [(m_me + k * width + i) % MID for i in range(width)]
        xs = [x_ref[pl.ds(m, REG, stride=MID), :] for m in ms]
        for x in xs:
            first = fold_squares(first, x)
        wide = mix_rows(h_mats[0], jnp.concatenate(xs, axis=1))
        tall = jnp.concatenate([wide[:, i * REG : (i + 1) * REG] for i in range(width)], axis=0)
        both = mix_lanes(tall, l01_mat[...])
        after = fold_squares(after, both[:, :REG])
        for i, m in enumerate(ms):
            pieces = block_transpose([both[i * REG + q * 32 : i * REG + (q + 1) * 32, REG:] for q in range(4)])
            for j in range(4):
                send1[pl.ds(pl.multiple_of((m * 4 + j) * 32, 32), 32), :] = pieces[j]

        @pl.when(k > 0)
        def _():
            send_chunk1(k - 1)

        return first, after

    first_sum, sum0 = lax.fori_loop(0, MID // width, section0, (zero, zero))
    send_chunk1(MID // width - 1)
    recv1[pl.ds(pl.multiple_of(me * 32, 32), 32), :] = send1[pl.ds(pl.multiple_of((m_me * 4 + j_me) * 32, 32), 32), :]

    send_gates(2)
    send_gates(3)
    pass_gates(2)
    pass_gates(3)
    end_gates(2)
    low2, high2 = compose(2)
    h_mats[2] = rows_cat(exact_dot(high2, from_split))
    l2_mat[...] = lanes_cat(low2.T)
    end_gates(3)
    low3, high3 = compose(3)
    h_mats[3] = rows_cat(exact_dot(to_split, exact_dot(high3, from_split)))
    l23_mat[...] = lanes_cat(exact_dot(low3, low2).T)

    def wait_bytes(ref, rows, sem):
        pltpu.make_async_copy(ref.at[pl.ds(0, rows)], ref.at[pl.ds(0, rows)], sem).wait()

    def split_rows(ref, index):
        return jnp.concatenate(
            [ref[pl.ds(2 * index, 64, stride=32), :], ref[pl.ds(2 * index + 1, 64, stride=32), :]], axis=0
        )

    wait_bytes(recv1, 63 * 32, recv1_sem)

    step = 4

    def section1(k, acc):
        rs = [k * step + i for i in range(step)]
        wide = mix_rows(h_mats[1], jnp.concatenate([split_rows(recv1, r) for r in rs], axis=1))
        acc = fold_squares(acc, wide[:, :REG])
        for i in range(1, step):
            acc = fold_squares(acc, wide[:, i * REG : (i + 1) * REG])
        for i, r in enumerate(rs):
            parts = block_transpose([wide[q * 32 : (q + 1) * 32, i * REG : (i + 1) * REG] for q in range(4)])
            for q in range(4):
                mid2[pl.ds(pl.multiple_of((q * 16 + r) * 32, 32), 32), :] = parts[q]
        return acc

    sum1 = lax.fori_loop(0, 16 // step, section1, zero)

    def section2(k, carry):
        ks = [k * step + i for i in range(step)]
        wide = mix_rows(h_mats[2], jnp.concatenate([split_rows(mid2, r) for r in ks], axis=1))
        for i, r in enumerate(ks):
            here = wide[:, i * REG : (i + 1) * REG]
            half2[pl.ds(pl.multiple_of(r * REG, REG), REG), :] = here
            parts = block_transpose([here[q * 32 : (q + 1) * 32] for q in range(4)])
            for q in range(4):
                mid3[pl.ds(pl.multiple_of((q * 16 + r) * 32, 32), 32), :] = parts[q]
        return carry

    lax.fori_loop(0, 16 // step, section2, 0)

    def send_half2(k, carry):
        j = (j_me + k) % 4
        pltpu.make_async_remote_copy(
            at(half2, j, 512), at(recv2, j_me, 512), send2_sem, recv2_sem,
            device_id=(seg, amp_of(m_me, j)), device_id_type=MESH,
        ).start()
        return carry

    lax.fori_loop(1, 4, send_half2, 0)

    def section3(k, carry):
        rs = [k * step + i for i in range(step)]
        wide = mix_rows(h_mats[3], jnp.concatenate([split_rows(mid3, r) for r in rs], axis=1))
        for i, r in enumerate(rs):
            here = wide[:, i * REG : (i + 1) * REG]
            send3[pl.ds(2 * r, 64, stride=32), :] = here[:64]
            send3[pl.ds(2 * r + 1, 64, stride=32), :] = here[64:]
        return carry

    lax.fori_loop(0, 16 // step, section3, 0)
    slot = m_me * 4 + j_me

    def send_piece3(k, carry):
        to = (me + k) % PEERS
        pltpu.make_async_remote_copy(
            at(send3, to, 32), at(recv3, slot, 32), send3_sem, recv3_sem, device_id=(seg, to), device_id_type=MESH
        ).start()
        return carry

    lax.fori_loop(1, PEERS, send_piece3, 0)
    recv3[pl.ds(pl.multiple_of(slot * 32, 32), 32), :] = send3[pl.ds(pl.multiple_of(me * 32, 32), 32), :]

    own = pl.ds(pl.multiple_of(j_me * 512, 512), 512)
    wait_bytes(recv2, 3 * 512, recv2_sem)
    recv2[own, :] = half2[own, :]

    def norm2(k, acc):
        parts = block_transpose(
            [recv2[pl.ds(pl.multiple_of(j * 512 + k * REG, REG), REG), :] for j in range(4)]
        )
        return fold_squares(acc, mix_lanes(jnp.concatenate(parts, axis=0), l2_mat[...]))

    sum2 = lax.fori_loop(0, 4, norm2, zero)
    wait_bytes(recv3, 63 * 32, recv3_sem)

    def last(k, acc):
        ms = [k * step + i for i in range(step)]
        tall = []
        for m in ms:
            tall += block_transpose([recv3[pl.ds(pl.multiple_of((m * 4 + j) * 32, 32), 32), :] for j in range(4)])
        mixed = mix_lanes(jnp.concatenate(tall, axis=0), l23_mat[...])
        for i, m in enumerate(ms):
            y_ref[pl.ds(m, REG, stride=MID), :] = mixed[i * REG : (i + 1) * REG]
        return fold_squares(acc, mixed)

    sum3 = lax.fori_loop(0, MID // step, last, zero)

    lane = lax.broadcasted_iota(jnp.int32, (1, REG), 1)
    line = jnp.zeros((1, REG), F32)
    for n, acc in enumerate((first_sum, sum0, sum1, sum2, sum3)):
        line = jnp.where(lane == n, jnp.sum(acc), line)
    sums_out[...] = line
    sums_in[me] = line

    def send_sums(k, carry):
        to = (me + k) % PEERS
        pltpu.make_async_remote_copy(
            sums_out, sums_in.at[me], sums_send, sums_recv, device_id=(seg, to), device_id_type=MESH
        ).start()
        return carry

    lax.fori_loop(1, PEERS, send_sums, 0)

    for section in range(SECTIONS):
        @pl.when(seg == section)
        def _():
            for k in range(1, SECTIONS):
                gate_copy(section, (seg + k) % SECTIONS).wait_send()

        @pl.when(seg != section)
        def _():
            pair_copy(section).wait_send()

    wait_bytes(send1, 63 * 32, send1_sem)
    wait_bytes(half2, 3 * 512, send2_sem)
    wait_bytes(send3, 63 * 32, send3_sem)
    wait_bytes(sums_in, 63, sums_send)
    wait_bytes(sums_in, 63, sums_recv)
    stats_ref[...] = jnp.sum(sums_in[...], axis=0)


def body(states, gate_blocks, kraus_picks, block_targets):
    amp_local = states.shape[1]
    total_amps = amp_local * lax.axis_size("amp")
    dma = pltpu.SemaphoreType.DMA
    vmem = pl.BlockSpec(memory_space=pltpu.VMEM)
    smem = pl.BlockSpec(memory_space=pltpu.SMEM)
    big = pltpu.VMEM((ROWS, REG), F32)
    values, totals = pl.pallas_call(
        kernel,
        out_shape=(jax.ShapeDtypeStruct((ROWS, REG), F32), jax.ShapeDtypeStruct((1, REG), F32)),
        in_specs=[vmem, vmem, smem, smem],
        out_specs=(vmem, vmem),
        scratch_shapes=[
            pltpu.VMEM((SECTIONS, BLOCKS, REG, REG), F32),
            big, big, big, big, big, big, big, big,
            pltpu.VMEM((SECTIONS, REG, 3 * REG), BF16),
            pltpu.VMEM((3 * REG, 2 * REG), BF16),
            pltpu.VMEM((3 * REG, REG), BF16),
            pltpu.VMEM((3 * REG, REG), BF16),
            pltpu.VMEM((1, REG), F32),
            pltpu.VMEM((PEERS, 1, REG), F32),
            dma((SECTIONS,)), dma((SECTIONS,)), dma((SECTIONS,)), dma((SECTIONS,)),
            dma, dma, dma, dma, dma, dma, dma, dma,
        ],
        compiler_params=pltpu.CompilerParams(collective_id=0, has_side_effects=True),
        name="trajectory",
    )(states.reshape(ROWS, REG), gate_blocks[0], kraus_picks[0], block_targets)
    totals = totals[0]
    log_weights = jnp.log(totals[1:5] / totals[0:4])
    scaled = values / jnp.sqrt(totals[4] / total_amps)
    return scaled.reshape(1, amp_local), log_weights.reshape(1, SECTIONS)


def solution(mesh):
    in_specs = (
        P("segment", "amp"),
        P("segment", None, None, None),
        P("segment", None, None, None),
        P(),
    )
    out_specs = (P("segment", "amp"), P("segment", None))
    return jax.shard_map(body, mesh=mesh, in_specs=in_specs, out_specs=out_specs, check_vma=False)
```

```python
import functools

import jax
import jax.numpy as jnp
from jax import lax
from jax.experimental import pallas as pl
from jax.experimental.pallas import tpu as pltpu
from jax.sharding import PartitionSpec as P

KEEP_FACTORS = (1.0, 0.9, 1.0, 0.97)
FLIP_FACTORS = (0.9, 1.0, 0.97, 1.0)
QUBITS = 7
REG = 128
MID = 16
PEERS = 64
SECTIONS = 4
BLOCKS = 3
ROWS = 2048
MESH = pl.DeviceIdType.MESH
F32 = jnp.float32
BF16 = jnp.bfloat16


def split(x):
    hi = x.astype(BF16)
    lo = (x - hi.astype(F32)).astype(BF16)
    return hi, lo


def exact_dot(a, b):
    return jnp.dot(a, b, precision=lax.Precision.HIGHEST, preferred_element_type=F32)


def mix_rows(gate_cat, x):
    hi, lo = split(x)
    return jnp.dot(gate_cat, jnp.concatenate([hi, hi, lo], axis=0), preferred_element_type=F32)


def mix_lanes(x, gate_cat):
    hi, lo = split(x)
    return jnp.dot(jnp.concatenate([hi, hi, lo], axis=1), gate_cat, preferred_element_type=F32)


def rows_cat(gate):
    hi, lo = split(gate)
    return jnp.concatenate([hi, lo, hi], axis=1)


def lanes_cat(gate_t):
    hi, lo = split(gate_t)
    return jnp.concatenate([hi, lo, hi], axis=0)


def block_transpose(arrays):
    lane = lax.broadcasted_iota(jnp.int32, arrays[0].shape, 1)
    low_half = lane < 64
    even = (lane // 32) % 2 == 0
    stage = [None] * 4
    for a in range(2):
        moved = pltpu.roll(jnp.where(low_half, arrays[a + 2], arrays[a]), 64, 1)
        stage[a] = jnp.where(low_half, arrays[a], moved)
        stage[a + 2] = jnp.where(low_half, moved, arrays[a + 2])
    result = [None] * 4
    for a in (0, 2):
        result[a] = jnp.where(even, stage[a], pltpu.roll(stage[a + 1], 32, 1))
        result[a + 1] = jnp.where(even, pltpu.roll(stage[a], 96, 1), stage[a + 1])
    return result


def fold_squares(acc, x):
    sq = x * x
    return acc + jnp.sum(sq.reshape(sq.shape[0] // 8, 8, sq.shape[1]), axis=0)


def amp_of(m, j):
    return (m // 8) * 32 + (j // 2) * 16 + (m % 8) * 2 + j % 2


def scalar_pick(kind, table):
    return jnp.where(
        kind == 0,
        F32(table[0]),
        jnp.where(kind == 1, F32(table[1]), jnp.where(kind == 2, F32(table[2]), F32(table[3]))),
    )


def kernel(
    x_ref, gate_ref, kraus_ref, target_ref,
    y_ref, scale_ref, logs_ref,
    all_gates, send1, recv1, mid1, mid2, mid3, recv2, wide2, send3, recv3, h_mats, l_mats, sums_out, sums_in,
    gate_send, gate_recv, pair_send, pair_recv,
    send1_sem, recv1_sem, send2_sem, recv2_sem, send3_sem, recv3_sem, sums_send, sums_recv,
):
    seg = lax.axis_index("segment")
    me = lax.axis_index("amp")
    y_me = me // 16
    z_me = (me % 16) // 2
    core = me % 2
    j_me = (y_me % 2) * 2 + core
    m_me = (y_me // 2) * 8 + z_me
    slot_me = m_me * 4 + j_me
    partner = me + 1 - 2 * core
    zero = jnp.zeros((8, REG), F32)

    def part(index, rows):
        return pl.ds(pl.multiple_of(index * rows, rows), rows)

    def wait_bytes(ref, rows, sem):
        pltpu.make_async_copy(ref.at[pl.ds(0, rows)], ref.at[pl.ds(0, rows)], sem).wait()

    barrier = pltpu.get_barrier_semaphore()

    def greet(k, carry):
        pl.semaphore_signal(barrier, inc=1, device_id=(seg, (me + k) % PEERS), device_id_type=MESH)
        return carry

    lax.fori_loop(1, PEERS, greet, 0)
    for k in range(1, SECTIONS):
        pl.semaphore_signal(barrier, inc=1, device_id=((seg + k) % SECTIONS, me), device_id_type=MESH)

    width = 4

    def pack(k, acc):
        for i in range(width):
            m = k * width + i
            x = x_ref[pl.ds(m, REG, stride=MID), :]
            acc = fold_squares(acc, x)
            pieces = block_transpose([x[q * 32 : (q + 1) * 32] for q in range(4)])
            for j in range(4):
                send1[part(m * 4 + j, 32), :] = pieces[j]
        return acc

    first_sum = lax.fori_loop(0, MID // width, pack, zero)
    all_gates[seg] = gate_ref[0]

    pl.semaphore_wait(barrier, PEERS - 1 + SECTIONS - 1)

    distances = (4, 5, 3, 6, 2, 7, 1, 0)

    def to_all(send_one):
        for dz in distances:
            def one(n, carry, dz=dz):
                z = (z_me + dz) % 8
                y = (y_me + n // 2) % 4
                c = (core + n) % 2
                send_one(y, z, c)
                return carry

            lax.fori_loop(0 if dz else 1, 8, one, 0)

    def send_piece1(y, z, c):
        piece = ((y // 2) * 8 + z) * 4 + (y % 2) * 2 + c
        pltpu.make_async_remote_copy(
            send1.at[part(piece, 32)], recv1.at[part(me, 32)], send1_sem, recv1_sem.at[z_me],
            device_id=(seg, y * 16 + z * 2 + c), device_id_type=MESH,
        ).start()

    to_all(send_piece1)
    recv1[part(me, 32), :] = send1[part(slot_me, 32), :]

    my_half = pl.ds(pl.multiple_of(core * 64, 64), 64)
    other_half = pl.ds(pl.multiple_of((1 - core) * 64, 64), 64)

    def gate_copy(section, target_seg):
        return pltpu.make_async_remote_copy(
            gate_ref.at[0, :, my_half, :],
            all_gates.at[section, :, my_half, :],
            gate_send.at[target_seg],
            gate_recv.at[section],
            device_id=(target_seg, me),
            device_id_type=MESH,
        )

    def pair_copy(section):
        return pltpu.make_async_remote_copy(
            all_gates.at[section, :, my_half, :],
            all_gates.at[section, :, my_half, :],
            pair_send.at[section],
            pair_recv.at[section],
            device_id=(seg, partner),
            device_id_type=MESH,
        )

    def send_gates(section):
        @pl.when(seg == section)
        def _():
            for k in range(1, SECTIONS):
                gate_copy(section, (seg + k) % SECTIONS).start()

    def pass_gates(section):
        @pl.when(seg != section)
        def _():
            gate_copy(section, section).wait_recv()
            pair_copy(section).start()

    def end_gates(section):
        @pl.when(seg != section)
        def _():
            pltpu.make_async_copy(
                all_gates.at[section, :, other_half, :], all_gates.at[section, :, other_half, :], pair_recv.at[section]
            ).wait()

    row = lax.broadcasted_iota(jnp.int32, (REG, REG), 0)
    col = lax.broadcasted_iota(jnp.int32, (REG, REG), 1)
    identity = (row == col).astype(F32)
    to_split = (col == (row % 64) * 2 + row // 64).astype(F32)
    from_split = (row == (col % 64) * 2 + col // 64).astype(F32)

    def noise(section, block):
        product = jnp.ones((REG, REG), F32)
        for q in range(QUBITS):
            kind = kraus_ref[0, section, block, q]
            bit = lax.shift_right_logical(row, QUBITS - 1 - q) & 1
            product = product * jnp.where(bit == 1, scalar_pick(kind, FLIP_FACTORS), scalar_pick(kind, KEEP_FACTORS))
        return product

    def compose(section):
        low, high = identity, identity
        for block in range(BLOCKS):
            on_low = target_ref[section, block] == 0
            gate = all_gates[section, block]
            if block == 0:
                mixed = gate
            else:
                mixed = exact_dot(gate, jnp.where(on_low, low, high))
            mixed = noise(section, block) * mixed
            low, high = jnp.where(on_low, mixed, low), jnp.where(on_low, high, mixed)
        return low, high

    for section in range(SECTIONS):
        send_gates(section)
    for section in range(SECTIONS):
        pass_gates(section)
    low_all = None
    for section in range(SECTIONS):
        end_gates(section)
        low, high = compose(section)
        if section > 0:
            high = exact_dot(high, from_split)
        if section == 3:
            high = exact_dot(to_split, high)
        h_mats[section] = rows_cat(high)
        low_all = low if section == 0 else exact_dot(low, low_all)
        l_mats[section] = lanes_cat(low_all.T)

    def split_rows(ref, index, stride, rows=64):
        return jnp.concatenate(
            [ref[pl.ds(2 * index, rows, stride=stride), :], ref[pl.ds(2 * index + 1, rows, stride=stride), :]], axis=0
        )

    def arrived(ref, sem, z):
        @pl.when(z == z_me)
        def _():
            wait_bytes(ref, 7 * 32, sem.at[z])

        @pl.when(z != z_me)
        def _():
            wait_bytes(ref, 8 * 32, sem.at[z])

    def source_z(k):
        dz = jnp.where(k % 2 == 1, 4 + (k + 1) // 2, 4 - k // 2)
        return (z_me + 8 - dz) % 8

    def section0(k, carry):
        z = source_z(k)
        arrived(recv1, recv1_sem, z)
        kappas = [z * 2, z * 2 + 1]
        tall = []
        for kappa in kappas:
            parts = block_transpose([recv1[part(y * 16 + kappa, 32), :] for y in range(4)])
            tall.append(jnp.concatenate(parts, axis=0))
        wide = mix_rows(h_mats[0], jnp.concatenate(tall, axis=1))
        for i, kappa in enumerate(kappas):
            parts = block_transpose([wide[q * 32 : (q + 1) * 32, i * REG : (i + 1) * REG] for q in range(4)])
            for y in range(4):
                mid1[part(y * 16 + kappa, 32), :] = parts[y]
        return carry

    lax.fori_loop(0, 8, section0, 0)
    step = 4

    def section1(k, carry):
        rs = [k * step + i for i in range(step)]
        wide = mix_rows(h_mats[1], jnp.concatenate([split_rows(mid1, r, 32) for r in rs], axis=1))
        for i, r in enumerate(rs):
            parts = block_transpose([wide[y * 32 : (y + 1) * 32, i * REG : (i + 1) * REG] for y in range(4)])
            for q in range(4):
                mid2[part(q * 16 + r, 32), :] = parts[q]
        return carry

    lax.fori_loop(0, 16 // step, section1, 0)

    def section2(k, carry):
        kappas = [k * step + i for i in range(step)]
        wide = mix_rows(h_mats[2], jnp.concatenate([split_rows(mid2, kappa, 32) for kappa in kappas], axis=1))
        for i, kappa in enumerate(kappas):
            parts = block_transpose([wide[q * 32 : (q + 1) * 32, i * REG : (i + 1) * REG] for q in range(4)])
            for y in range(4):
                mid3[part(y * 16 + kappa, 32), :] = parts[y]
        return carry

    lax.fori_loop(0, 16 // step, section2, 0)

    mid2_tiles = mid2.reshape(64, 32, REG)
    recv2_tiles = recv2.reshape(4, 64, 8, REG)

    def send_quarter(k, carry):
        j = (j_me + k) % 4
        pltpu.make_async_remote_copy(
            mid2_tiles.at[:, part(j, 8), :], recv2_tiles.at[j_me], send2_sem, recv2_sem,
            device_id=(seg, (m_me // 8) * 32 + (j // 2) * 16 + z_me * 2 + j % 2), device_id_type=MESH,
        ).start()
        return carry

    lax.fori_loop(1, 4, send_quarter, 0)

    def section3(k, carry):
        rs = [k * step + i for i in range(step)]
        wide = mix_rows(h_mats[3], jnp.concatenate([split_rows(mid3, r, 32) for r in rs], axis=1))
        for i, r in enumerate(rs):
            here = wide[:, i * REG : (i + 1) * REG]
            send3[pl.ds(2 * r, 64, stride=32), :] = here[:64]
            send3[pl.ds(2 * r + 1, 64, stride=32), :] = here[64:]
        return carry

    lax.fori_loop(0, 16 // step, section3, 0)

    def send_piece3(y, z, c):
        to = y * 16 + z * 2 + c
        pltpu.make_async_remote_copy(
            send3.at[part(to, 32)], recv3.at[part(slot_me, 32)], send3_sem, recv3_sem.at[z_me],
            device_id=(seg, to), device_id_type=MESH,
        ).start()

    to_all(send_piece3)
    recv3[part(slot_me, 32), :] = send3[part(me, 32), :]

    def norm0(k, acc):
        xs = [x_ref[pl.ds(k * step + i, REG, stride=MID), :] for i in range(step)]
        wide = mix_rows(h_mats[0], jnp.concatenate(xs, axis=1))
        tall = jnp.concatenate([wide[:, i * REG : (i + 1) * REG] for i in range(step)], axis=0)
        return fold_squares(acc, mix_lanes(tall, l_mats[0]))

    sum0 = lax.fori_loop(0, MID // step, norm0, zero)
    wait_bytes(recv2, 3 * 512, recv2_sem)
    for n in range(4):
        recv2_tiles[j_me, n * 16 : (n + 1) * 16] = mid2_tiles[n * 16 : (n + 1) * 16, part(j_me, 8), :]

    def norm1(k, acc):
        parts = block_transpose([recv2[part(j * 4 + k, REG), :] for j in range(4)])
        for y in range(4):
            wide2[part(y * 4 + k, REG), :] = parts[y]
        return fold_squares(acc, mix_lanes(jnp.concatenate(parts, axis=0), l_mats[1]))

    sum1 = lax.fori_loop(0, 4, norm1, zero)

    def norm2(k, acc):
        xs = [split_rows(wide2.at[part(k, 512)], i, 8) for i in range(4)]
        wide = mix_rows(h_mats[2], jnp.concatenate(xs, axis=1))
        tall = jnp.concatenate([wide[:, i * REG : (i + 1) * REG] for i in range(4)], axis=0)
        return fold_squares(acc, mix_lanes(tall, l_mats[2]))

    sum2 = lax.fori_loop(0, 4, norm2, zero)

    def last(k, acc):
        z = source_z(k)
        arrived(recv3, recv3_sem, z)
        ms = [z, z + 8]
        tall = []
        for m in ms:
            tall += block_transpose([recv3[part(m * 4 + j, 32), :] for j in range(4)])
        mixed = mix_lanes(jnp.concatenate(tall, axis=0), l_mats[3])
        for i, m in enumerate(ms):
            y_ref[pl.ds(m, REG, stride=MID), :] = mixed[i * REG : (i + 1) * REG]
        return fold_squares(acc, mixed)

    sum3 = lax.fori_loop(0, 8, last, zero)

    lane = lax.broadcasted_iota(jnp.int32, (1, REG), 1)
    line = jnp.ones((1, REG), F32)
    for n, acc in enumerate((first_sum, sum0, sum1, sum2, sum3)):
        line = jnp.where(lane == n, jnp.sum(acc), line)
    sums_out[...] = line
    sums_in[me] = line

    def send_sums(y, z, c):
        pltpu.make_async_remote_copy(
            sums_out, sums_in.at[me], sums_send, sums_recv, device_id=(seg, y * 16 + z * 2 + c), device_id_type=MESH
        ).start()

    to_all(send_sums)

    for section in range(SECTIONS):
        @pl.when(seg == section)
        def _():
            for k in range(1, SECTIONS):
                gate_copy(section, (seg + k) % SECTIONS).wait_send()

        @pl.when(seg != section)
        def _():
            pair_copy(section).wait_send()

    wait_bytes(send1, 63 * 32, send1_sem)
    wait_bytes(recv2, 3 * 512, send2_sem)
    wait_bytes(send3, 63 * 32, send3_sem)
    wait_bytes(sums_in, 63, sums_send)
    wait_bytes(sums_in, 63, sums_recv)
    totals = jnp.sum(sums_in[...], axis=0)
    logs_ref[...] = jnp.log(pltpu.roll(totals, REG - 1, 1) / totals)
    mean = jnp.sum(jnp.where(lane == 4, totals, 0.0)) / (PEERS * ROWS * REG)
    scale_ref[...] = 1.0 / jnp.sqrt(jnp.full((1, REG), mean, F32))


def body(states, gate_blocks, kraus_picks, block_targets):
    dma = pltpu.SemaphoreType.DMA
    vmem = pl.BlockSpec(memory_space=pltpu.VMEM)
    smem = pl.BlockSpec(memory_space=pltpu.SMEM)
    big = pltpu.VMEM((ROWS, REG), F32)
    line = jax.ShapeDtypeStruct((1, REG), F32)
    values, scale, logs = pl.pallas_call(
        kernel,
        out_shape=(jax.ShapeDtypeStruct((ROWS, REG), F32), line, line),
        in_specs=[vmem, vmem, smem, smem],
        out_specs=(vmem, vmem, vmem),
        scratch_shapes=[
            pltpu.VMEM((SECTIONS, BLOCKS, REG, REG), F32),
            big, big, big, big, big, big, big, big, big,
            pltpu.VMEM((SECTIONS, REG, 3 * REG), BF16),
            pltpu.VMEM((SECTIONS, 3 * REG, REG), BF16),
            pltpu.VMEM((1, REG), F32),
            pltpu.VMEM((PEERS, 1, REG), F32),
            dma((SECTIONS,)), dma((SECTIONS,)), dma((SECTIONS,)), dma((SECTIONS,)),
            dma, dma((8,)), dma, dma, dma, dma((8,)), dma, dma,
        ],
        compiler_params=pltpu.CompilerParams(collective_id=0, has_side_effects=True),
        name="trajectory",
    )(states.reshape(ROWS, REG), gate_blocks, kraus_picks, block_targets)
    return (values * scale).reshape(states.shape), logs[:, :SECTIONS]


def solution(mesh):
    in_specs = (
        P("segment", "amp"),
        P("segment", None, None, None),
        P("segment", None, None, None),
        P(),
    )
    out_specs = (P("segment", "amp"), P("segment", None))
    return jax.shard_map(body, mesh=mesh, in_specs=in_specs, out_specs=out_specs, check_vma=False)
```

```python
import functools

import jax
import jax.numpy as jnp
from jax import lax
from jax.experimental import pallas as pl
from jax.experimental.pallas import tpu as pltpu
from jax.sharding import PartitionSpec as P

KEEP_FACTORS = (1.0, 0.9, 1.0, 0.97)
FLIP_FACTORS = (0.9, 1.0, 0.97, 1.0)
QUBITS = 7
REG = 128
MID = 16
PEERS = 64
SECTIONS = 4
BLOCKS = 3
ROWS = 2048
MESH = pl.DeviceIdType.MESH
F32 = jnp.float32
BF16 = jnp.bfloat16


def split(x):
    hi = x.astype(BF16)
    lo = (x - hi.astype(F32)).astype(BF16)
    return hi, lo


def exact_dot(a, b):
    return jnp.dot(a, b, precision=lax.Precision.HIGHEST, preferred_element_type=F32)


def mix_rows(gate_cat, x):
    hi, lo = split(x)
    return jnp.dot(gate_cat, jnp.concatenate([hi, hi, lo], axis=0), preferred_element_type=F32)


def mix_lanes(x, gate_cat):
    hi, lo = split(x)
    return jnp.dot(jnp.concatenate([hi, hi, lo], axis=1), gate_cat, preferred_element_type=F32)


def rows_cat(gate):
    hi, lo = split(gate)
    return jnp.concatenate([hi, lo, hi], axis=1)


def lanes_cat(gate_t):
    hi, lo = split(gate_t)
    return jnp.concatenate([hi, lo, hi], axis=0)


def block_transpose(arrays):
    lane = lax.broadcasted_iota(jnp.int32, arrays[0].shape, 1)
    low_half = lane < 64
    even = (lane // 32) % 2 == 0
    stage = [None] * 4
    for a in range(2):
        moved = pltpu.roll(jnp.where(low_half, arrays[a + 2], arrays[a]), 64, 1)
        stage[a] = jnp.where(low_half, arrays[a], moved)
        stage[a + 2] = jnp.where(low_half, moved, arrays[a + 2])
    result = [None] * 4
    for a in (0, 2):
        result[a] = jnp.where(even, stage[a], pltpu.roll(stage[a + 1], 32, 1))
        result[a + 1] = jnp.where(even, pltpu.roll(stage[a], 96, 1), stage[a + 1])
    return result


def fold_squares(acc, x):
    sq = x * x
    return acc + jnp.sum(sq.reshape(sq.shape[0] // 8, 8, sq.shape[1]), axis=0)


def amp_of(m, j):
    return (m // 8) * 32 + (j // 2) * 16 + (m % 8) * 2 + j % 2


def scalar_pick(kind, table):
    return jnp.where(
        kind == 0,
        F32(table[0]),
        jnp.where(kind == 1, F32(table[1]), jnp.where(kind == 2, F32(table[2]), F32(table[3]))),
    )


def kernel(
    states_ref, gate_ref, kraus_ref, target_ref,
    y_ref, scale_ref, logs_ref,
    x_ref, all_gates, send1, recv1, mid1, mid2, mid3, recv2, wide2, send3, recv3, h_mats, l_mats, sums_out, sums_in,
    gate_send, gate_recv, pair_send, pair_recv,
    send1_sem, recv1_sem, send2_sem, recv2_sem, send3_sem, recv3_sem, sums_send, sums_recv,
    load_sems,
):
    seg = lax.axis_index("segment")
    me = lax.axis_index("amp")
    y_me = me // 16
    z_me = (me % 16) // 2
    core = me % 2
    j_me = (y_me % 2) * 2 + core
    m_me = (y_me // 2) * 8 + z_me
    slot_me = m_me * 4 + j_me
    partner = me + 1 - 2 * core
    zero = jnp.zeros((8, REG), F32)

    def part(index, rows):
        return pl.ds(pl.multiple_of(index * rows, rows), rows)

    def wait_bytes(ref, rows, sem):
        pltpu.make_async_copy(ref.at[pl.ds(0, rows)], ref.at[pl.ds(0, rows)], sem).wait()

    load_states = pltpu.make_async_copy(states_ref, x_ref, load_sems.at[0])
    load_gates = pltpu.make_async_copy(gate_ref.at[0], all_gates.at[seg], load_sems.at[1])
    load_states.start()
    load_gates.start()

    distances = (4, 5, 3, 6, 2, 7, 1, 0)

    def to_all(send_one, wanted=distances):
        for dz in wanted:
            def one(n, carry, dz=dz):
                send_one((y_me + n // 2) % 4, (z_me + dz) % 8, (core + n) % 2)
                return carry

            lax.fori_loop(0 if dz else 1, 8, one, 0)

    barrier = pltpu.get_barrier_semaphore()

    def greet(y, z, c):
        pl.semaphore_signal(barrier, inc=1, device_id=(seg, y * 16 + z * 2 + c), device_id_type=MESH)

    to_all(greet)
    for k in range(1, SECTIONS):
        pl.semaphore_signal(barrier, inc=1, device_id=((seg + k) % SECTIONS, me), device_id_type=MESH)

    width = 4

    def pack(k, acc):
        for i in range(width):
            m = k * width + i
            x = x_ref[pl.ds(m, REG, stride=MID), :]
            acc = fold_squares(acc, x)
            pieces = block_transpose([x[q * 32 : (q + 1) * 32] for q in range(4)])
            for j in range(4):
                send1[part(m * 4 + j, 32), :] = pieces[j]
        return acc

    load_states.wait()
    first_sum = lax.fori_loop(0, MID // width, pack, zero)
    load_gates.wait()

    pl.semaphore_wait(barrier, PEERS - 1 + SECTIONS - 1)

    def exchange(source, target, piece_of, slot, send_sem, recv_sem):
        def one(y, z, c):
            pltpu.make_async_remote_copy(
                source.at[part(piece_of(y, z, c), 32)], target.at[part(slot, 32)], send_sem, recv_sem.at[z_me],
                device_id=(seg, y * 16 + z * 2 + c), device_id_type=MESH,
            ).start()

        to_all(one)

    def piece_by_m(y, z, c):
        return ((y // 2) * 8 + z) * 4 + (y % 2) * 2 + c

    def piece_by_g(y, z, c):
        return y * 16 + z * 2 + c

    exchange(send1, recv1, piece_by_m, me, send1_sem, recv1_sem)
    recv1[part(me, 32), :] = send1[part(slot_me, 32), :]

    my_half = pl.ds(pl.multiple_of(core * 64, 64), 64)
    other_half = pl.ds(pl.multiple_of((1 - core) * 64, 64), 64)

    def gate_copy(section, target_seg):
        return pltpu.make_async_remote_copy(
            all_gates.at[section, :, my_half, :],
            all_gates.at[section, :, my_half, :],
            gate_send.at[target_seg],
            gate_recv.at[section],
            device_id=(target_seg, me),
            device_id_type=MESH,
        )

    def pair_copy(section):
        return pltpu.make_async_remote_copy(
            all_gates.at[section, :, my_half, :],
            all_gates.at[section, :, my_half, :],
            pair_send.at[section],
            pair_recv.at[section],
            device_id=(seg, partner),
            device_id_type=MESH,
        )

    def send_gates(section):
        @pl.when(seg == section)
        def _():
            for k in range(1, SECTIONS):
                gate_copy(section, (seg + k) % SECTIONS).start()

    def pass_gates(section):
        @pl.when(seg != section)
        def _():
            gate_copy(section, section).wait_recv()
            pair_copy(section).start()

    def end_gates(section):
        @pl.when(seg != section)
        def _():
            pltpu.make_async_copy(
                all_gates.at[section, :, other_half, :], all_gates.at[section, :, other_half, :], pair_recv.at[section]
            ).wait()

    row = lax.broadcasted_iota(jnp.int32, (REG, REG), 0)
    col = lax.broadcasted_iota(jnp.int32, (REG, REG), 1)
    identity = (row == col).astype(F32)
    to_split = (col == (row % 64) * 2 + row // 64).astype(F32)
    from_split = (row == (col % 64) * 2 + col // 64).astype(F32)

    def noise(section, block):
        product = jnp.ones((REG, REG), F32)
        for q in range(QUBITS):
            kind = kraus_ref[0, block, section, q]
            bit = lax.shift_right_logical(row, QUBITS - 1 - q) & 1
            product = product * jnp.where(bit == 1, scalar_pick(kind, FLIP_FACTORS), scalar_pick(kind, KEEP_FACTORS))
        return product

    def compose(section):
        low, high = identity, identity
        for block in range(BLOCKS):
            on_low = target_ref[section, block] == 0
            gate = all_gates[section, block]
            if block == 0:
                mixed = gate
            else:
                mixed = exact_dot(gate, jnp.where(on_low, low, high))
            mixed = noise(section, block) * mixed
            low, high = jnp.where(on_low, mixed, low), jnp.where(on_low, high, mixed)
        return low, high

    for section in range(SECTIONS):
        send_gates(section)
    for section in range(SECTIONS):
        pass_gates(section)
    low_all = None
    for section in range(SECTIONS):
        end_gates(section)
        low, high = compose(section)
        if section > 0:
            high = exact_dot(high, from_split)
        if section == 3:
            high = exact_dot(to_split, high)
        h_mats[section] = rows_cat(high)
        low_all = low if section == 0 else exact_dot(low, low_all)
        l_mats[section] = lanes_cat(low_all.T)

    def split_rows(ref, index, stride, rows=64):
        return jnp.concatenate(
            [ref[pl.ds(2 * index, rows, stride=stride), :], ref[pl.ds(2 * index + 1, rows, stride=stride), :]], axis=0
        )

    def arrived(ref, sem, z):
        @pl.when(z == z_me)
        def _():
            wait_bytes(ref, 7 * 32, sem.at[z])

        @pl.when(z != z_me)
        def _():
            wait_bytes(ref, 8 * 32, sem.at[z])

    def source_z(k):
        dz = jnp.where(k % 2 == 1, 4 + (k + 1) // 2, 4 - k // 2)
        return (z_me + 8 - dz) % 8

    def section0(k, carry):
        z = source_z(k)
        arrived(recv1, recv1_sem, z)
        kappas = [z * 2, z * 2 + 1]
        tall = []
        for kappa in kappas:
            parts = block_transpose([recv1[part(y * 16 + kappa, 32), :] for y in range(4)])
            tall.append(jnp.concatenate(parts, axis=0))
        wide = mix_rows(h_mats[0], jnp.concatenate(tall, axis=1))
        for i, kappa in enumerate(kappas):
            parts = block_transpose([wide[q * 32 : (q + 1) * 32, i * REG : (i + 1) * REG] for q in range(4)])
            for y in range(4):
                mid1[part(y * 16 + kappa, 32), :] = parts[y]
        return carry

    lax.fori_loop(0, 8, section0, 0)
    step = 4

    def section1(k, carry):
        rs = [k * step + i for i in range(step)]
        wide = mix_rows(h_mats[1], jnp.concatenate([split_rows(mid1, r, 32) for r in rs], axis=1))
        for i, r in enumerate(rs):
            parts = block_transpose([wide[y * 32 : (y + 1) * 32, i * REG : (i + 1) * REG] for y in range(4)])
            for q in range(4):
                mid2[part(q * 16 + r, 32), :] = parts[q]
        return carry

    lax.fori_loop(0, 16 // step, section1, 0)

    def section2(k, carry):
        kappas = [k * step + i for i in range(step)]
        wide = mix_rows(h_mats[2], jnp.concatenate([split_rows(mid2, kappa, 32) for kappa in kappas], axis=1))
        for i, kappa in enumerate(kappas):
            parts = block_transpose([wide[q * 32 : (q + 1) * 32, i * REG : (i + 1) * REG] for q in range(4)])
            for y in range(4):
                mid3[part(y * 16 + kappa, 32), :] = parts[y]
        return carry

    lax.fori_loop(0, 16 // step, section2, 0)

    mid2_tiles = mid2.reshape(64, 32, REG)
    recv2_tiles = recv2.reshape(4, 64, 8, REG)

    def send_quarter(k, carry):
        j = (j_me + k) % 4
        pltpu.make_async_remote_copy(
            mid2_tiles.at[:, part(j, 8), :], recv2_tiles.at[j_me], send2_sem, recv2_sem,
            device_id=(seg, (m_me // 8) * 32 + (j // 2) * 16 + z_me * 2 + j % 2), device_id_type=MESH,
        ).start()
        return carry

    lax.fori_loop(1, 4, send_quarter, 0)

    def section3(k, carry):
        rs = [k * step + i for i in range(step)]
        wide = mix_rows(h_mats[3], jnp.concatenate([split_rows(mid3, r, 32) for r in rs], axis=1))
        for i, r in enumerate(rs):
            here = wide[:, i * REG : (i + 1) * REG]
            send3[pl.ds(2 * r, 64, stride=32), :] = here[:64]
            send3[pl.ds(2 * r + 1, 64, stride=32), :] = here[64:]
        return carry

    lax.fori_loop(0, 16 // step, section3, 0)

    exchange(send3, recv3, piece_by_g, slot_me, send3_sem, recv3_sem)
    recv3[part(slot_me, 32), :] = send3[part(me, 32), :]

    def norm0(k, acc):
        xs = [x_ref[pl.ds(k * step + i, REG, stride=MID), :] for i in range(step)]
        wide = mix_rows(h_mats[0], jnp.concatenate(xs, axis=1))
        tall = jnp.concatenate([wide[:, i * REG : (i + 1) * REG] for i in range(step)], axis=0)
        return fold_squares(acc, mix_lanes(tall, l_mats[0]))

    sum0 = lax.fori_loop(0, MID // step, norm0, zero)
    wait_bytes(recv2, 3 * 512, recv2_sem)
    for n in range(4):
        recv2_tiles[j_me, n * 16 : (n + 1) * 16] = mid2_tiles[n * 16 : (n + 1) * 16, part(j_me, 8), :]

    def norm1(k, acc):
        parts = block_transpose([recv2[part(j * 4 + k, REG), :] for j in range(4)])
        for y in range(4):
            wide2[part(y * 4 + k, REG), :] = parts[y]
        return fold_squares(acc, mix_lanes(jnp.concatenate(parts, axis=0), l_mats[1]))

    sum1 = lax.fori_loop(0, 4, norm1, zero)

    def norm2(k, acc):
        xs = [split_rows(wide2.at[part(k, 512)], i, 8) for i in range(4)]
        wide = mix_rows(h_mats[2], jnp.concatenate(xs, axis=1))
        tall = jnp.concatenate([wide[:, i * REG : (i + 1) * REG] for i in range(4)], axis=0)
        return fold_squares(acc, mix_lanes(tall, l_mats[2]))

    sum2 = lax.fori_loop(0, 4, norm2, zero)

    def last(k, acc):
        z = source_z(k)
        arrived(recv3, recv3_sem, z)
        ms = [z, z + 8]
        tall = []
        for m in ms:
            tall += block_transpose([recv3[part(m * 4 + j, 32), :] for j in range(4)])
        mixed = mix_lanes(jnp.concatenate(tall, axis=0), l_mats[3])
        for i, m in enumerate(ms):
            y_ref[pl.ds(m, REG, stride=MID), :] = mixed[i * REG : (i + 1) * REG]
        return fold_squares(acc, mixed)

    sum3 = lax.fori_loop(0, 8, last, zero)

    lane = lax.broadcasted_iota(jnp.int32, (1, REG), 1)
    line = jnp.ones((1, REG), F32)
    for n, acc in enumerate((first_sum, sum0, sum1, sum2, sum3)):
        line = jnp.where(lane == n, jnp.sum(acc), line)
    sums_out[...] = line
    sums_in[me] = line

    def send_sums(y, z, c):
        pltpu.make_async_remote_copy(
            sums_out, sums_in.at[me], sums_send, sums_recv, device_id=(seg, y * 16 + z * 2 + c), device_id_type=MESH
        ).start()

    to_all(send_sums)

    for section in range(SECTIONS):
        @pl.when(seg == section)
        def _():
            for k in range(1, SECTIONS):
                gate_copy(section, (seg + k) % SECTIONS).wait_send()

        @pl.when(seg != section)
        def _():
            pair_copy(section).wait_send()

    wait_bytes(send1, 63 * 32, send1_sem)
    wait_bytes(recv2, 3 * 512, send2_sem)
    wait_bytes(send3, 63 * 32, send3_sem)
    wait_bytes(sums_in, 63, sums_send)
    wait_bytes(sums_in, 63, sums_recv)
    totals = jnp.sum(sums_in[...], axis=0)
    logs_ref[...] = jnp.log(pltpu.roll(totals, REG - 1, 1) / totals)
    mean = jnp.sum(jnp.where(lane == 4, totals, 0.0)) / (PEERS * ROWS * REG)
    scale_ref[...] = 1.0 / jnp.sqrt(jnp.full((1, REG), mean, F32))


def scale_kernel(values_ref, scale_ref, logs_ref, y_ref, log_weights_ref, scaled, sems):
    log_weights_ref[...] = logs_ref[:, :SECTIONS]
    rows = ROWS // 4
    for n in range(4):
        part = pl.ds(n * rows, rows)
        scaled[part, :] = values_ref[part, :] * scale_ref[...]
        pltpu.make_async_copy(scaled.at[part], y_ref.at[part], sems.at[n]).start()
    for n in range(4):
        part = pl.ds(n * rows, rows)
        pltpu.make_async_copy(scaled.at[part], y_ref.at[part], sems.at[n]).wait()


def body(states, gate_blocks, kraus_picks, block_targets):
    dma = pltpu.SemaphoreType.DMA
    vmem = pl.BlockSpec(memory_space=pltpu.VMEM)
    smem = pl.BlockSpec(memory_space=pltpu.SMEM)
    anywhere = pl.BlockSpec(memory_space=pl.ANY)
    big = pltpu.VMEM((ROWS, REG), F32)
    line = pltpu.VMEM((1, REG), F32)
    values, scale, logs = pl.pallas_call(
        kernel,
        out_shape=(big, line, line),
        in_specs=[anywhere, anywhere, smem, smem],
        out_specs=(vmem, vmem, vmem),
        scratch_shapes=[
            big,
            pltpu.VMEM((SECTIONS, BLOCKS, REG, REG), F32),
            big, big, big, big, big, big, big, big, big,
            pltpu.VMEM((SECTIONS, REG, 3 * REG), BF16),
            pltpu.VMEM((SECTIONS, 3 * REG, REG), BF16),
            pltpu.VMEM((1, REG), F32),
            pltpu.VMEM((PEERS, 1, REG), F32),
            dma((SECTIONS,)), dma((SECTIONS,)), dma((SECTIONS,)), dma((SECTIONS,)),
            dma, dma((8,)), dma, dma, dma, dma((8,)), dma, dma,
            dma((2,)),
        ],
        compiler_params=pltpu.CompilerParams(collective_id=0, has_side_effects=True),
        name="trajectory",
    )(states.reshape(ROWS, REG), gate_blocks, kraus_picks.transpose(0, 2, 1, 3), block_targets)
    final, log_weights = pl.pallas_call(
        scale_kernel,
        out_shape=(jax.ShapeDtypeStruct((ROWS, REG), F32), jax.ShapeDtypeStruct((1, SECTIONS), F32)),
        in_specs=[vmem, vmem, vmem],
        out_specs=(anywhere, vmem),
        scratch_shapes=[big, dma((4,))],
        compiler_params=pltpu.CompilerParams(vmem_limit_bytes=8 * 2**20),
        name="scale",
    )(values, scale, logs)
    return final.reshape(states.shape), log_weights


def solution(mesh):
    in_specs = (
        P("segment", "amp"),
        P("segment", None, None, None),
        P("segment", None, None, None),
        P(),
    )
    out_specs = (P("segment", "amp"), P("segment", None))
    return jax.shard_map(body, mesh=mesh, in_specs=in_specs, out_specs=out_specs, check_vma=False)
```

```python
import functools

import jax
import jax.numpy as jnp
from jax import lax
from jax.experimental import pallas as pl
from jax.experimental.pallas import tpu as pltpu
from jax.sharding import PartitionSpec as P

KEEP_FACTORS = (1.0, 0.9, 1.0, 0.97)
FLIP_FACTORS = (0.9, 1.0, 0.97, 1.0)
QUBITS = 7
REG = 128
MID = 16
PEERS = 64
SECTIONS = 4
BLOCKS = 3
ROWS = 2048
MESH = pl.DeviceIdType.MESH
F32 = jnp.float32
BF16 = jnp.bfloat16


def split(x):
    hi = x.astype(BF16)
    lo = (x - hi.astype(F32)).astype(BF16)
    return hi, lo


def exact_dot(a, b):
    return jnp.dot(a, b, precision=lax.Precision.HIGHEST, preferred_element_type=F32)


def mix_rows(gate_cat, x):
    hi, lo = split(x)
    return jnp.dot(gate_cat, jnp.concatenate([hi, hi, lo], axis=0), preferred_element_type=F32)


def mix_lanes(x, gate_cat):
    hi, lo = split(x)
    return jnp.dot(jnp.concatenate([hi, hi, lo], axis=1), gate_cat, preferred_element_type=F32)


def rows_cat(gate):
    hi, lo = split(gate)
    return jnp.concatenate([hi, lo, hi], axis=1)


def lanes_cat(gate_t):
    hi, lo = split(gate_t)
    return jnp.concatenate([hi, lo, hi], axis=0)


def block_transpose(arrays):
    lane = lax.broadcasted_iota(jnp.int32, arrays[0].shape, 1)
    low_half = lane < 64
    even = (lane // 32) % 2 == 0
    stage = [None] * 4
    for a in range(2):
        moved = pltpu.roll(jnp.where(low_half, arrays[a + 2], arrays[a]), 64, 1)
        stage[a] = jnp.where(low_half, arrays[a], moved)
        stage[a + 2] = jnp.where(low_half, moved, arrays[a + 2])
    result = [None] * 4
    for a in (0, 2):
        result[a] = jnp.where(even, stage[a], pltpu.roll(stage[a + 1], 32, 1))
        result[a + 1] = jnp.where(even, pltpu.roll(stage[a], 96, 1), stage[a + 1])
    return result


def fold_squares(acc, x):
    sq = x * x
    return acc + jnp.sum(sq.reshape(sq.shape[0] // 8, 8, sq.shape[1]), axis=0)


def amp_of(m, j):
    return (m // 8) * 32 + (j // 2) * 16 + (m % 8) * 2 + j % 2


def scalar_pick(kind, table):
    return jnp.where(
        kind == 0,
        F32(table[0]),
        jnp.where(kind == 1, F32(table[1]), jnp.where(kind == 2, F32(table[2]), F32(table[3]))),
    )


def kernel(
    states_ref, gate_ref, kraus_hbm, target_hbm,
    y_ref, scale_ref, logs_ref,
    kraus_ref, target_ref, x_ref, all_gates, send1, recv1, mid1, mid2, mid3, recv2, wide2, send3, recv3, h_mats, l_mats, sums_out, sums_in,
    gate_send, gate_recv, pair_send, pair_recv,
    send1_sem, recv1_sem, send2_sem, recv2_sem, send3_sem, recv3_sem, sums_send, sums_recv,
    load_sems,
):
    seg = lax.axis_index("segment")
    me = lax.axis_index("amp")
    y_me = me // 16
    z_me = (me % 16) // 2
    core = me % 2
    j_me = (y_me % 2) * 2 + core
    m_me = (y_me // 2) * 8 + z_me
    slot_me = m_me * 4 + j_me
    kappa_me = me // 4
    partner = me + 1 - 2 * core
    zero = jnp.zeros((8, REG), F32)

    def part(index, rows):
        return pl.ds(pl.multiple_of(index * rows, rows), rows)

    def wait_bytes(ref, rows, sem):
        pltpu.make_async_copy(ref.at[pl.ds(0, rows)], ref.at[pl.ds(0, rows)], sem).wait()

    loads = [
        pltpu.make_async_copy(states_ref, x_ref, load_sems.at[0]),
        pltpu.make_async_copy(gate_ref.at[0], all_gates.at[seg], load_sems.at[1]),
        pltpu.make_async_copy(kraus_hbm, kraus_ref, load_sems.at[2]),
        pltpu.make_async_copy(target_hbm, target_ref, load_sems.at[3]),
    ]
    for load in loads:
        load.start()

    barrier = pltpu.get_barrier_semaphore()

    def greet(k, carry):
        pl.semaphore_signal(barrier, inc=1, device_id=(seg, (me + k) % PEERS), device_id_type=MESH)
        return carry

    lax.fori_loop(40, PEERS, greet, 0)
    lax.fori_loop(1, 40, greet, 0)
    for k in range(1, SECTIONS):
        pl.semaphore_signal(barrier, inc=1, device_id=((seg + k) % SECTIONS, me), device_id_type=MESH)

    far_first = ((1, 0), (1, 1), (0, 1), (0, 0))
    near_first = far_first[::-1]

    def to_all(send_one, flips=far_first):
        for flip_upper, flip_lower in flips:
            y = ((y_me // 2 + flip_upper) % 2) * 2 + (y_me + flip_lower) % 2
            for on in (2, 1, 3, 0):
                pair = (z_me // 2 + on) % 4

                def one(n, carry, y=y, pair=pair):
                    send_one(y, pair * 2 + (z_me + n // 2) % 2, (core + n) % 2)
                    return carry

                lax.fori_loop(0 if flip_upper or flip_lower or on else 1, 4, one, 0)

    width = 16

    def pack(k, acc):
        for i in range(width):
            m = k * width + i
            x = x_ref[pl.ds(m, REG, stride=MID), :]
            acc = fold_squares(acc, x)
            pieces = block_transpose([x[q * 32 : (q + 1) * 32] for q in range(4)])
            for j in range(4):
                send1[part(m * 4 + j, 32), :] = pieces[j]
        return acc

    loads[0].wait()
    first_sum = lax.fori_loop(0, MID // width, pack, zero)
    for load in loads[1:]:
        load.wait()

    pl.semaphore_wait(barrier, PEERS - 1 + SECTIONS - 1)

    def exchange(source, target, piece_of, slot, send_sem, recv_sem, group, flips):
        def one(y, z, c):
            pltpu.make_async_remote_copy(
                source.at[part(piece_of(y, z, c), 32)], target.at[part(slot, 32)], send_sem, recv_sem.at[group],
                device_id=(seg, y * 16 + z * 2 + c), device_id_type=MESH,
            ).start()

        to_all(one, flips)

    def piece_by_m(y, z, c):
        return ((y // 2) * 8 + z) * 4 + (y % 2) * 2 + c

    def piece_by_g(y, z, c):
        return y * 16 + z * 2 + c

    exchange(send1, recv1, piece_by_m, me, send1_sem, recv1_sem, kappa_me, far_first)
    recv1[part(me, 32), :] = send1[part(slot_me, 32), :]

    my_half = pl.ds(pl.multiple_of(core * 64, 64), 64)
    other_half = pl.ds(pl.multiple_of((1 - core) * 64, 64), 64)

    def gate_copy(section, target_seg):
        return pltpu.make_async_remote_copy(
            all_gates.at[section, :, my_half, :],
            all_gates.at[section, :, my_half, :],
            gate_send.at[target_seg],
            gate_recv.at[section],
            device_id=(target_seg, me),
            device_id_type=MESH,
        )

    def pair_copy(section):
        return pltpu.make_async_remote_copy(
            all_gates.at[section, :, my_half, :],
            all_gates.at[section, :, my_half, :],
            pair_send.at[section],
            pair_recv.at[section],
            device_id=(seg, partner),
            device_id_type=MESH,
        )

    def send_gates(section):
        @pl.when(seg == section)
        def _():
            for k in range(1, SECTIONS):
                gate_copy(section, (seg + k) % SECTIONS).start()

    def pass_gates(section):
        @pl.when(seg != section)
        def _():
            gate_copy(section, section).wait_recv()
            pair_copy(section).start()

    def end_gates(section):
        @pl.when(seg != section)
        def _():
            pltpu.make_async_copy(
                all_gates.at[section, :, other_half, :], all_gates.at[section, :, other_half, :], pair_recv.at[section]
            ).wait()

    row = lax.broadcasted_iota(jnp.int32, (REG, REG), 0)
    col = lax.broadcasted_iota(jnp.int32, (REG, REG), 1)
    identity = (row == col).astype(F32)
    to_split = (col == (row % 64) * 2 + row // 64).astype(F32)
    from_split = (row == (col % 64) * 2 + col // 64).astype(F32)
    to_lanes = (col == (row % 32 // 2) * 8 + (row // 32) * 2 + row % 2).astype(F32)

    def noise(section, block):
        product = jnp.ones((REG, REG), F32)
        for q in range(QUBITS):
            kind = kraus_ref[0, block, section, q]
            bit = lax.shift_right_logical(row, QUBITS - 1 - q) & 1
            product = product * jnp.where(bit == 1, scalar_pick(kind, FLIP_FACTORS), scalar_pick(kind, KEEP_FACTORS))
        return product

    def compose(section):
        low, high = identity, identity
        for block in range(BLOCKS):
            on_low = target_ref[section, block] == 0
            gate = all_gates[section, block]
            if block == 0:
                mixed = gate
            else:
                mixed = exact_dot(gate, jnp.where(on_low, low, high))
            mixed = noise(section, block) * mixed
            low, high = jnp.where(on_low, mixed, low), jnp.where(on_low, high, mixed)
        return low, high

    for section in range(SECTIONS):
        send_gates(section)
    for section in range(SECTIONS):
        pass_gates(section)
    low_all = None
    for section in range(SECTIONS):
        end_gates(section)
        low, high = compose(section)
        if section > 0:
            high = exact_dot(high, from_split)
        if section % 2 == 1:
            high = exact_dot(to_lanes if section == 1 else to_split, high)
        h_mats[section] = rows_cat(high)
        low_all = low if section == 0 else exact_dot(low, low_all)
        l_mats[section] = lanes_cat(low_all.T)

    def split_rows(ref, index, stride, rows=64):
        return jnp.concatenate(
            [ref[pl.ds(2 * index, rows, stride=stride), :], ref[pl.ds(2 * index + 1, rows, stride=stride), :]], axis=0
        )

    def arrived(ref, sem, group, own):
        @pl.when(group == own)
        def _():
            wait_bytes(ref, 3 * 32, sem.at[group])

        @pl.when(group != own)
        def _():
            wait_bytes(ref, 4 * 32, sem.at[group])

    def section0(k, carry):
        flip, half = k // 2, k % 2
        y = ((y_me // 2 + 1 - flip // 2) % 2) * 2 + (y_me + (flip + 1) // 2) % 2
        kappas = [y * 4 + (z_me // 2 + 4 - on) % 4 for on in (2 + half, 1 - half)]
        tall = []
        for kappa in kappas:
            arrived(recv1, recv1_sem, kappa, kappa_me)
            parts = block_transpose([recv1[part(kappa * 4 + n, 32), :] for n in range(4)])
            tall.append(jnp.concatenate(parts, axis=0))
        wide = mix_rows(h_mats[0], jnp.concatenate(tall, axis=1))
        for i, kappa in enumerate(kappas):
            parts = block_transpose([wide[q * 32 : (q + 1) * 32, i * REG : (i + 1) * REG] for q in range(4)])
            for n in range(4):
                mid1[part(kappa * 4 + n, 32), :] = parts[n]
        return carry

    lax.fori_loop(0, 8, section0, 0)
    step = 16

    def section1(k, carry):
        rs = [k * step + i for i in range(step)]
        wide = mix_rows(h_mats[1], jnp.concatenate([split_rows(mid1, r, 32) for r in rs], axis=1))
        for i, r in enumerate(rs):
            parts = block_transpose([wide[n * 32 : (n + 1) * 32, i * REG : (i + 1) * REG] for n in range(4)])
            for q in range(4):
                mid2[part(q * 16 + r, 32), :] = parts[q]
        return carry

    lax.fori_loop(0, 16 // step, section1, 0)

    def section2(k, carry):
        kappas = [k * step + i for i in range(step)]
        wide = mix_rows(h_mats[2], jnp.concatenate([split_rows(mid2, kappa, 32) for kappa in kappas], axis=1))
        for i, kappa in enumerate(kappas):
            parts = block_transpose([wide[q * 32 : (q + 1) * 32, i * REG : (i + 1) * REG] for q in range(4)])
            for n in range(4):
                mid3[part(kappa * 4 + n, 32), :] = parts[n]
        return carry

    lax.fori_loop(0, 16 // step, section2, 0)

    mid2_tiles = mid2.reshape(64, 32, REG)
    recv2_tiles = recv2.reshape(4, 64, 8, REG)

    def send_quarter(k, carry):
        j = (j_me + k) % 4
        pltpu.make_async_remote_copy(
            mid2_tiles.at[:, part(j, 8), :], recv2_tiles.at[j_me], send2_sem, recv2_sem,
            device_id=(seg, (m_me // 8) * 32 + (j // 2) * 16 + z_me * 2 + j % 2), device_id_type=MESH,
        ).start()
        return carry

    lax.fori_loop(1, 4, send_quarter, 0)

    def section3(k, carry):
        rs = [k * step + i for i in range(step)]
        wide = mix_rows(h_mats[3], jnp.concatenate([split_rows(mid3, r, 32) for r in rs], axis=1))
        for i, r in enumerate(rs):
            here = wide[:, i * REG : (i + 1) * REG]
            send3[pl.ds(2 * r, 64, stride=32), :] = here[:64]
            send3[pl.ds(2 * r + 1, 64, stride=32), :] = here[64:]
        return carry

    lax.fori_loop(0, 16 // step, section3, 0)

    exchange(send3, recv3, piece_by_g, slot_me, send3_sem, recv3_sem, m_me, near_first)
    recv3[part(slot_me, 32), :] = send3[part(me, 32), :]

    step = 4

    def norm0(k, acc):
        xs = [x_ref[pl.ds(k * step + i, REG, stride=MID), :] for i in range(step)]
        wide = mix_rows(h_mats[0], jnp.concatenate(xs, axis=1))
        tall = jnp.concatenate([wide[:, i * REG : (i + 1) * REG] for i in range(step)], axis=0)
        return fold_squares(acc, mix_lanes(tall, l_mats[0]))

    sum0 = lax.fori_loop(0, MID // step, norm0, zero)
    wait_bytes(recv2, 3 * 512, recv2_sem)
    for n in range(4):
        recv2_tiles[j_me, n * 16 : (n + 1) * 16] = mid2_tiles[n * 16 : (n + 1) * 16, part(j_me, 8), :]

    def norm1(k, acc):
        parts = block_transpose([recv2[part(j * 4 + k, REG), :] for j in range(4)])
        for y in range(4):
            wide2[part(y * 4 + k, REG), :] = parts[y]
        return fold_squares(acc, mix_lanes(jnp.concatenate(parts, axis=0), l_mats[1]))

    sum1 = lax.fori_loop(0, 4, norm1, zero)

    def norm2(k, acc):
        xs = [split_rows(wide2.at[part(k, 512)], i, 8) for i in range(4)]
        wide = mix_rows(h_mats[2], jnp.concatenate(xs, axis=1))
        tall = jnp.concatenate([wide[:, i * REG : (i + 1) * REG] for i in range(4)], axis=0)
        return fold_squares(acc, mix_lanes(tall, l_mats[2]))

    sum2 = lax.fori_loop(0, 4, norm2, zero)

    def last(k, acc):
        on = k % 4
        pair = (z_me // 2 + jnp.where(on < 2, on + 2, 3 - on)) % 4
        upper = (y_me // 2 + k // 4) % 2
        ms = [upper * 8 + pair * 2, upper * 8 + pair * 2 + 1]
        tall = []
        for m in ms:
            arrived(recv3, recv3_sem, m, m_me)
            tall += block_transpose([recv3[part(m * 4 + j, 32), :] for j in range(4)])
        mixed = mix_lanes(jnp.concatenate(tall, axis=0), l_mats[3])
        for i, m in enumerate(ms):
            y_ref[pl.ds(m, REG, stride=MID), :] = mixed[i * REG : (i + 1) * REG]
        return fold_squares(acc, mixed)

    sum3 = lax.fori_loop(0, 8, last, zero)

    lane = lax.broadcasted_iota(jnp.int32, (1, REG), 1)
    line = jnp.ones((1, REG), F32)
    for n, acc in enumerate((first_sum, sum0, sum1, sum2, sum3)):
        line = jnp.where(lane == n, jnp.sum(acc), line)
    sums_out[...] = line
    sums_in[me] = line

    def send_sums(y, z, c):
        pltpu.make_async_remote_copy(
            sums_out, sums_in.at[me], sums_send, sums_recv, device_id=(seg, y * 16 + z * 2 + c), device_id_type=MESH
        ).start()

    to_all(send_sums)

    for section in range(SECTIONS):
        @pl.when(seg == section)
        def _():
            for k in range(1, SECTIONS):
                gate_copy(section, (seg + k) % SECTIONS).wait_send()

        @pl.when(seg != section)
        def _():
            pair_copy(section).wait_send()

    wait_bytes(send1, 63 * 32, send1_sem)
    wait_bytes(recv2, 3 * 512, send2_sem)
    wait_bytes(send3, 63 * 32, send3_sem)
    wait_bytes(sums_in, 63, sums_send)
    wait_bytes(sums_in, 63, sums_recv)
    totals = jnp.sum(sums_in[...], axis=0)
    logs_ref[...] = jnp.log(pltpu.roll(totals, REG - 1, 1) / totals)
    mean = jnp.sum(jnp.where(lane == 4, totals, 0.0)) / (PEERS * ROWS * REG)
    scale_ref[...] = 1.0 / jnp.sqrt(jnp.full((1, REG), mean, F32))


def scale_kernel(values_ref, scale_ref, logs_ref, y_ref, log_weights_ref, scaled, sems):
    log_weights_ref[...] = logs_ref[:, :SECTIONS]
    rows = ROWS // 4
    for n in range(4):
        part = pl.ds(n * rows, rows)
        scaled[part, :] = values_ref[part, :] * scale_ref[...]
        pltpu.make_async_copy(scaled.at[part], y_ref.at[part], sems.at[n]).start()
    for n in range(4):
        part = pl.ds(n * rows, rows)
        pltpu.make_async_copy(scaled.at[part], y_ref.at[part], sems.at[n]).wait()


def body(states, gate_blocks, kraus_picks, block_targets):
    dma = pltpu.SemaphoreType.DMA
    vmem = pl.BlockSpec(memory_space=pltpu.VMEM)
    anywhere = pl.BlockSpec(memory_space=pl.ANY)
    big = pltpu.VMEM((ROWS, REG), F32)
    line = pltpu.VMEM((1, REG), F32)
    values, scale, logs = pl.pallas_call(
        kernel,
        out_shape=(big, line, line),
        in_specs=[anywhere] * 4,
        out_specs=(vmem, vmem, vmem),
        scratch_shapes=[
            pltpu.SMEM((1, BLOCKS, SECTIONS, QUBITS), jnp.int32),
            pltpu.SMEM((SECTIONS, BLOCKS), jnp.int32),
            big,
            pltpu.VMEM((SECTIONS, BLOCKS, REG, REG), F32),
            big, big, big, big, big, big, big, big, big,
            pltpu.VMEM((SECTIONS, REG, 3 * REG), BF16),
            pltpu.VMEM((SECTIONS, 3 * REG, REG), BF16),
            pltpu.VMEM((1, REG), F32),
            pltpu.VMEM((PEERS, 1, REG), F32),
            dma((SECTIONS,)), dma((SECTIONS,)), dma((SECTIONS,)), dma((SECTIONS,)),
            dma, dma((16,)), dma, dma, dma, dma((16,)), dma, dma,
            dma((4,)),
        ],
        compiler_params=pltpu.CompilerParams(collective_id=0, has_side_effects=True),
        name="trajectory",
    )(states.reshape(ROWS, REG), gate_blocks, kraus_picks.transpose(0, 2, 1, 3), block_targets)
    final, log_weights = pl.pallas_call(
        scale_kernel,
        out_shape=(jax.ShapeDtypeStruct((ROWS, REG), F32), jax.ShapeDtypeStruct((1, SECTIONS), F32)),
        in_specs=[vmem, vmem, vmem],
        out_specs=(anywhere, vmem),
        scratch_shapes=[big, dma((4,))],
        compiler_params=pltpu.CompilerParams(vmem_limit_bytes=8 * 2**20),
        name="scale",
    )(values, scale, logs)
    return final.reshape(states.shape), log_weights


def solution(mesh):
    in_specs = (
        P("segment", "amp"),
        P("segment", None, None, None),
        P("segment", None, None, None),
        P(),
    )
    out_specs = (P("segment", "amp"), P("segment", None))
    return jax.shard_map(body, mesh=mesh, in_specs=in_specs, out_specs=out_specs, check_vma=False)
```

```python
import functools

import jax
import jax.numpy as jnp
from jax import lax
from jax.experimental import pallas as pl
from jax.experimental.pallas import tpu as pltpu
from jax.sharding import PartitionSpec as P

KEEP_FACTORS = (1.0, 0.9, 1.0, 0.97)
FLIP_FACTORS = (0.9, 1.0, 0.97, 1.0)
QUBITS = 7
REG = 128
MID = 16
PEERS = 64
SECTIONS = 4
BLOCKS = 3
ROWS = 2048
MESH = pl.DeviceIdType.MESH
F32 = jnp.float32
BF16 = jnp.bfloat16


def split(x):
    hi = x.astype(BF16)
    lo = (x - hi.astype(F32)).astype(BF16)
    return hi, lo


def exact_dot(a, b):
    return jnp.dot(a, b, precision=lax.Precision.HIGHEST, preferred_element_type=F32)


def mix_rows(gate_cat, x):
    hi, lo = split(x)
    return jnp.dot(gate_cat, jnp.concatenate([hi, hi, lo], axis=0), preferred_element_type=F32)


def mix_lanes(x, gate_cat):
    hi, lo = split(x)
    return jnp.dot(jnp.concatenate([hi, hi, lo], axis=1), gate_cat, preferred_element_type=F32)


def rows_cat(gate):
    hi, lo = split(gate)
    return jnp.concatenate([hi, lo, hi], axis=1)


def lanes_cat(gate_t):
    hi, lo = split(gate_t)
    return jnp.concatenate([hi, lo, hi], axis=0)


def block_transpose(arrays):
    block = lax.broadcasted_iota(jnp.int32, arrays[0].shape, 1) // 16
    for bit in (4, 2, 1):
        low = (block // bit) % 2 == 0
        after = list(arrays)
        for a in range(8):
            if a & bit:
                continue
            here, there = arrays[a], arrays[a + bit]
            if bit == 4:
                moved = pltpu.roll(jnp.where(low, there, here), 64, 1)
                after[a] = jnp.where(low, here, moved)
                after[a + bit] = jnp.where(low, moved, there)
            else:
                after[a] = jnp.where(low, here, pltpu.roll(there, 16 * bit, 1))
                after[a + bit] = jnp.where(low, pltpu.roll(here, REG - 16 * bit, 1), there)
        arrays = after
    return arrays


def fold_squares(acc, x):
    sq = x * x
    return acc + jnp.sum(sq.reshape(sq.shape[0] // 8, 8, sq.shape[1]), axis=0)


def amp_of(m, j):
    return (m // 8) * 32 + (j // 2) * 16 + (m % 8) * 2 + j % 2


def scalar_pick(kind, table):
    return jnp.where(
        kind == 0,
        F32(table[0]),
        jnp.where(kind == 1, F32(table[1]), jnp.where(kind == 2, F32(table[2]), F32(table[3]))),
    )


def kernel(
    states_ref, gate_ref, kraus_hbm, target_hbm,
    y_ref, scale_ref, logs_ref,
    kraus_ref, target_ref, x_ref, all_gates, send1, recv1, mid1, mid2, mid3, quarters, recv2, wide2, send3, recv3, h_mats, l_mats, sums_out, sums_in,
    gate_send, gate_recv, pair_send, pair_recv,
    send1_sem, recv1_sem, send2_sem, recv2_sem, send3_sem, recv3_sem, sums_send, sums_recv,
    load_sems,
):
    seg = lax.axis_index("segment")
    me = lax.axis_index("amp")
    y_me = me // 16
    z_me = (me % 16) // 2
    core = me % 2
    j_me = (y_me % 2) * 2 + core
    m_me = (y_me // 2) * 8 + z_me
    slot_me = m_me * 4 + j_me
    kappa_me = me // 8
    partner = me + 1 - 2 * core
    zero = jnp.zeros((8, REG), F32)

    def part(index, rows):
        return pl.ds(pl.multiple_of(index * rows, rows), rows)

    def wait_bytes(ref, rows, sem):
        pltpu.make_async_copy(ref.at[pl.ds(0, rows)], ref.at[pl.ds(0, rows)], sem).wait()

    loads = [
        pltpu.make_async_copy(states_ref, x_ref, load_sems.at[0]),
        pltpu.make_async_copy(gate_ref.at[0], all_gates.at[seg], load_sems.at[1]),
        pltpu.make_async_copy(kraus_hbm, kraus_ref, load_sems.at[2]),
        pltpu.make_async_copy(target_hbm, target_ref, load_sems.at[3]),
    ]
    for load in loads:
        load.start()

    barrier = pltpu.get_barrier_semaphore()

    def greet(k, carry):
        pl.semaphore_signal(barrier, inc=1, device_id=(seg, (me + k) % PEERS), device_id_type=MESH)
        return carry

    lax.fori_loop(40, PEERS, greet, 0)
    lax.fori_loop(1, 40, greet, 0)
    for k in range(1, SECTIONS):
        pl.semaphore_signal(barrier, inc=1, device_id=((seg + k) % SECTIONS, me), device_id_type=MESH)

    far_first = ((1, 0), (1, 1), (0, 1), (0, 0))
    near_first = far_first[::-1]

    def to_all(send_one, flips=far_first):
        for flip_upper, flip_lower in flips:
            y = ((y_me // 2 + flip_upper) % 2) * 2 + (y_me + flip_lower) % 2
            for on in (1, 0):
                half = (z_me // 4 + on) % 2

                def one(n, carry, y=y, half=half):
                    send_one(y, half * 4 + (z_me + n // 2) % 4, (core + n) % 2)
                    return carry

                lax.fori_loop(0 if flip_upper or flip_lower or on else 1, 8, one, 0)

    width = 16

    def pack(k, acc):
        for i in range(width):
            m = k * width + i
            x = x_ref[pl.ds(m, REG, stride=MID), :]
            acc = fold_squares(acc, x)
            pieces = block_transpose([x[q * 16 : (q + 1) * 16] for q in range(8)])
            for b in range(8):
                send1[part(b % 2 * 64 + m * 4 + b // 2, 16), :] = pieces[b]
        return acc

    loads[0].wait()
    first_sum = lax.fori_loop(0, MID // width, pack, zero)
    for load in loads[1:]:
        load.wait()

    pl.semaphore_wait(barrier, PEERS - 1 + SECTIONS - 1)

    def exchange(e, source, target, piece_of, slot, send_sem, recv_sem, group, flips):
        def one(y, z, c):
            pltpu.make_async_remote_copy(
                source.at[part(e * 64 + piece_of(y, z, c), 16)], target.at[part(e * 64 + slot, 16)],
                send_sem, recv_sem.at[group],
                device_id=(seg, y * 16 + z * 2 + c), device_id_type=MESH,
            ).start()

        to_all(one, flips)

    def piece_by_m(y, z, c):
        return ((y // 2) * 8 + z) * 4 + (y % 2) * 2 + c

    def piece_by_g(y, z, c):
        return y * 16 + z * 2 + c

    for e in range(2):
        exchange(e, send1, recv1, piece_by_m, me, send1_sem, recv1_sem, e * 8 + kappa_me, far_first)
    for e in range(2):
        recv1[part(e * 64 + me, 16), :] = send1[part(e * 64 + slot_me, 16), :]

    my_half = pl.ds(pl.multiple_of(core * 64, 64), 64)
    other_half = pl.ds(pl.multiple_of((1 - core) * 64, 64), 64)

    def gate_copy(section, target_seg):
        return pltpu.make_async_remote_copy(
            all_gates.at[section, :, my_half, :],
            all_gates.at[section, :, my_half, :],
            gate_send.at[target_seg],
            gate_recv.at[section],
            device_id=(target_seg, me),
            device_id_type=MESH,
        )

    def pair_copy(section):
        return pltpu.make_async_remote_copy(
            all_gates.at[section, :, my_half, :],
            all_gates.at[section, :, my_half, :],
            pair_send.at[section],
            pair_recv.at[section],
            device_id=(seg, partner),
            device_id_type=MESH,
        )

    def send_gates(section):
        @pl.when(seg == section)
        def _():
            for k in range(1, SECTIONS):
                gate_copy(section, (seg + k) % SECTIONS).start()

    def pass_gates(section):
        @pl.when(seg != section)
        def _():
            gate_copy(section, section).wait_recv()
            pair_copy(section).start()

    def end_gates(section):
        @pl.when(seg != section)
        def _():
            pltpu.make_async_copy(
                all_gates.at[section, :, other_half, :], all_gates.at[section, :, other_half, :], pair_recv.at[section]
            ).wait()

    row = lax.broadcasted_iota(jnp.int32, (REG, REG), 0)
    col = lax.broadcasted_iota(jnp.int32, (REG, REG), 1)
    identity = (row == col).astype(F32)
    to_split = (col == (row % 64) * 2 + row // 64).astype(F32)
    from_split = (row == (col % 64) * 2 + col // 64).astype(F32)
    to_lanes = (col == (row % 16 // 2) * 16 + (row // 16) * 2 + row % 2).astype(F32)

    def noise(section, block):
        product = jnp.ones((REG, REG), F32)
        for q in range(QUBITS):
            kind = kraus_ref[0, block, section, q]
            bit = lax.shift_right_logical(row, QUBITS - 1 - q) & 1
            product = product * jnp.where(bit == 1, scalar_pick(kind, FLIP_FACTORS), scalar_pick(kind, KEEP_FACTORS))
        return product

    def compose(section):
        low, high = identity, identity
        for block in range(BLOCKS):
            on_low = target_ref[section, block] == 0
            gate = all_gates[section, block]
            if block == 0:
                mixed = gate
            else:
                mixed = exact_dot(gate, jnp.where(on_low, low, high))
            mixed = noise(section, block) * mixed
            low, high = jnp.where(on_low, mixed, low), jnp.where(on_low, high, mixed)
        return low, high

    for section in range(SECTIONS):
        send_gates(section)
    for section in range(SECTIONS):
        pass_gates(section)
    low_all = None
    for section in range(SECTIONS):
        end_gates(section)
        low, high = compose(section)
        if section > 0:
            high = exact_dot(high, from_split)
        if section % 2 == 1:
            high = exact_dot(to_lanes if section == 1 else to_split, high)
        h_mats[section] = rows_cat(high)
        low_all = low if section == 0 else exact_dot(low, low_all)
        l_mats[section] = lanes_cat(low_all.T)

    def split_rows(ref, index, stride, rows=64):
        return jnp.concatenate(
            [ref[pl.ds(2 * index, rows, stride=stride), :], ref[pl.ds(2 * index + 1, rows, stride=stride), :]], axis=0
        )

    def arrived(ref, sem, group, own, pieces):
        @pl.when(own)
        def _():
            wait_bytes(ref, (pieces - 1) * 16, sem.at[group])

        @pl.when(jnp.logical_not(own))
        def _():
            wait_bytes(ref, pieces * 16, sem.at[group])

    def chunk(wide, i, n):
        return wide[n * 16 : (n + 1) * 16, i * REG : (i + 1) * REG]

    def section0(e):
        def some(k, carry):
            y = ((y_me // 2 + 1 - k // 2) % 2) * 2 + (y_me + (k + 1) // 2) % 2
            kappas = [y * 2 + (z_me // 4 + on) % 2 for on in (1, 0)]
            tall = []
            for kappa in kappas:
                arrived(recv1, recv1_sem, e * 8 + kappa, kappa == kappa_me, 8)
                parts = block_transpose([recv1[part(e * 64 + kappa * 8 + n, 16), :] for n in range(8)])
                tall.append(jnp.concatenate(parts, axis=0))
            wide = mix_rows(h_mats[0], jnp.concatenate(tall, axis=1))
            for i, kappa in enumerate(kappas):
                parts = block_transpose([chunk(wide, i, q) for q in range(8)])
                for n in range(8):
                    mid1[part(e * 64 + kappa * 8 + n, 16), :] = parts[n]
            return carry

        lax.fori_loop(0, 4, some, 0)

    def half_rows(ref, e):
        return ref.at[pl.ds(e * 1024, 1024)]

    def section1(e):
        source = half_rows(mid1, e)
        wide = mix_rows(h_mats[1], jnp.concatenate([split_rows(source, r, 16) for r in range(8)], axis=1))
        for r in range(8):
            parts = block_transpose([chunk(wide, r, n) for n in range(8)])
            for q in range(8):
                mid2[part(e * 64 + q * 8 + r, 16), :] = parts[q]
                for j in range(4):
                    quarters[pl.ds(((j * 2 + e) * 64 + q * 8 + r) * 4, 4), :] = parts[q][j * 4 : (j + 1) * 4]

    def section2(e):
        source = half_rows(mid2, e)
        wide = mix_rows(h_mats[2], jnp.concatenate([split_rows(source, kappa, 16) for kappa in range(8)], axis=1))
        for kappa in range(8):
            parts = block_transpose([chunk(wide, kappa, q) for q in range(8)])
            for n in range(8):
                mid3[part(e * 64 + kappa * 8 + n, 16), :] = parts[n]

    def section3(e):
        source = half_rows(mid3, e)
        wide = mix_rows(h_mats[3], jnp.concatenate([split_rows(source, r, 16) for r in range(8)], axis=1))
        target = half_rows(send3, e)
        for r in range(8):
            here = wide[:, r * REG : (r + 1) * REG]
            target[pl.ds(2 * r, 64, stride=16), :] = here[:64]
            target[pl.ds(2 * r + 1, 64, stride=16), :] = here[64:]

    def send_quarters(e):
        def one(k, carry):
            j = (j_me + k) % 4
            pltpu.make_async_remote_copy(
                quarters.at[part(j * 2 + e, 256)], recv2.at[part(j_me * 2 + e, 256)], send2_sem, recv2_sem,
                device_id=(seg, (m_me // 8) * 32 + (j // 2) * 16 + z_me * 2 + j % 2), device_id_type=MESH,
            ).start()
            return carry

        lax.fori_loop(1, 4, one, 0)

    for e in range(2):
        section0(e)
        section1(e)
        section2(e)
        send_quarters(e)
        section3(e)
        exchange(e, send3, recv3, piece_by_g, slot_me, send3_sem, recv3_sem, e * 16 + m_me, near_first)
        recv3[part(e * 64 + slot_me, 16), :] = send3[part(e * 64 + me, 16), :]

    step = 4

    def norm0(k, acc):
        xs = [x_ref[pl.ds(k * step + i, REG, stride=MID), :] for i in range(step)]
        wide = mix_rows(h_mats[0], jnp.concatenate(xs, axis=1))
        tall = jnp.concatenate([wide[:, i * REG : (i + 1) * REG] for i in range(step)], axis=0)
        return fold_squares(acc, mix_lanes(tall, l_mats[0]))

    sum0 = lax.fori_loop(0, MID // step, norm0, zero)
    wait_bytes(recv2, 3 * 512, recv2_sem)
    recv2[part(j_me, 512), :] = quarters[part(j_me, 512), :]

    def norm1(k, acc):
        parts = block_transpose([recv2[pl.ds(pl.multiple_of(b * 256 + k * 64, 64), 64), :] for b in range(8)])
        for n in range(8):
            wide2[pl.ds(pl.multiple_of(n * 256 + k * 64, 64), 64), :] = parts[n]
        return fold_squares(acc, mix_lanes(jnp.concatenate(parts, axis=0), l_mats[1]))

    sum1 = lax.fori_loop(0, 4, norm1, zero)

    def norm2(k, acc):
        xs = [split_rows(wide2.at[part(2 * k + i // 2, 256)], i % 2, 4) for i in range(4)]
        wide = mix_rows(h_mats[2], jnp.concatenate(xs, axis=1))
        tall = jnp.concatenate([wide[:, i * REG : (i + 1) * REG] for i in range(4)], axis=0)
        return fold_squares(acc, mix_lanes(tall, l_mats[2]))

    sum2 = lax.fori_loop(0, 4, norm2, zero)

    def last(k, acc):
        upper = (y_me // 2 + k // 4) % 2
        z = ((z_me // 4 + 1 - k % 4 // 2) % 2) * 4 + 2 * (k % 2)
        ms = [upper * 8 + z, upper * 8 + z + 1]
        tall = []
        for m in ms:
            for e in range(2):
                arrived(recv3, recv3_sem, e * 16 + m, m == m_me, 4)
            tall += block_transpose([recv3[part(b % 2 * 64 + m * 4 + b // 2, 16), :] for b in range(8)])
        mixed = mix_lanes(jnp.concatenate(tall, axis=0), l_mats[3])
        for i, m in enumerate(ms):
            y_ref[pl.ds(m, REG, stride=MID), :] = mixed[i * REG : (i + 1) * REG]
        return fold_squares(acc, mixed)

    sum3 = lax.fori_loop(0, 8, last, zero)

    lane = lax.broadcasted_iota(jnp.int32, (1, REG), 1)
    line = jnp.ones((1, REG), F32)
    for n, acc in enumerate((first_sum, sum0, sum1, sum2, sum3)):
        line = jnp.where(lane == n, jnp.sum(acc), line)
    sums_out[...] = line
    sums_in[me] = line

    def send_sums(y, z, c):
        pltpu.make_async_remote_copy(
            sums_out, sums_in.at[me], sums_send, sums_recv, device_id=(seg, y * 16 + z * 2 + c), device_id_type=MESH
        ).start()

    to_all(send_sums)

    for section in range(SECTIONS):
        @pl.when(seg == section)
        def _():
            for k in range(1, SECTIONS):
                gate_copy(section, (seg + k) % SECTIONS).wait_send()

        @pl.when(seg != section)
        def _():
            pair_copy(section).wait_send()

    wait_bytes(send1, 126 * 16, send1_sem)
    wait_bytes(recv2, 3 * 512, send2_sem)
    wait_bytes(send3, 126 * 16, send3_sem)
    wait_bytes(sums_in, 63, sums_send)
    wait_bytes(sums_in, 63, sums_recv)
    totals = jnp.sum(sums_in[...], axis=0)
    logs_ref[...] = jnp.log(pltpu.roll(totals, REG - 1, 1) / totals)
    mean = jnp.sum(jnp.where(lane == 4, totals, 0.0)) / (PEERS * ROWS * REG)
    scale_ref[...] = 1.0 / jnp.sqrt(jnp.full((1, REG), mean, F32))


def scale_kernel(values_ref, scale_ref, logs_ref, y_ref, log_weights_ref, scaled, sems):
    log_weights_ref[...] = logs_ref[:, :SECTIONS]
    rows = ROWS // 4
    for n in range(4):
        part = pl.ds(n * rows, rows)
        scaled[part, :] = values_ref[part, :] * scale_ref[...]
        pltpu.make_async_copy(scaled.at[part], y_ref.at[part], sems.at[n]).start()
    for n in range(4):
        part = pl.ds(n * rows, rows)
        pltpu.make_async_copy(scaled.at[part], y_ref.at[part], sems.at[n]).wait()


def body(states, gate_blocks, kraus_picks, block_targets):
    dma = pltpu.SemaphoreType.DMA
    vmem = pl.BlockSpec(memory_space=pltpu.VMEM)
    anywhere = pl.BlockSpec(memory_space=pl.ANY)
    big = pltpu.VMEM((ROWS, REG), F32)
    line = pltpu.VMEM((1, REG), F32)
    values, scale, logs = pl.pallas_call(
        kernel,
        out_shape=(big, line, line),
        in_specs=[anywhere] * 4,
        out_specs=(vmem, vmem, vmem),
        scratch_shapes=[
            pltpu.SMEM((1, BLOCKS, SECTIONS, QUBITS), jnp.int32),
            pltpu.SMEM((SECTIONS, BLOCKS), jnp.int32),
            big,
            pltpu.VMEM((SECTIONS, BLOCKS, REG, REG), F32),
            big, big, big, big, big, big, big, big, big, big,
            pltpu.VMEM((SECTIONS, REG, 3 * REG), BF16),
            pltpu.VMEM((SECTIONS, 3 * REG, REG), BF16),
            pltpu.VMEM((1, REG), F32),
            pltpu.VMEM((PEERS, 1, REG), F32),
            dma((SECTIONS,)), dma((SECTIONS,)), dma((SECTIONS,)), dma((SECTIONS,)),
            dma, dma((16,)), dma, dma, dma, dma((32,)), dma, dma,
            dma((4,)),
        ],
        compiler_params=pltpu.CompilerParams(collective_id=0, has_side_effects=True),
        name="trajectory",
    )(states.reshape(ROWS, REG), gate_blocks, kraus_picks.transpose(0, 2, 1, 3), block_targets)
    final, log_weights = pl.pallas_call(
        scale_kernel,
        out_shape=(jax.ShapeDtypeStruct((ROWS, REG), F32), jax.ShapeDtypeStruct((1, SECTIONS), F32)),
        in_specs=[vmem, vmem, vmem],
        out_specs=(anywhere, vmem),
        scratch_shapes=[big, dma((4,))],
        compiler_params=pltpu.CompilerParams(vmem_limit_bytes=8 * 2**20),
        name="scale",
    )(values, scale, logs)
    return final.reshape(states.shape), log_weights


def solution(mesh):
    in_specs = (
        P("segment", "amp"),
        P("segment", None, None, None),
        P("segment", None, None, None),
        P(),
    )
    out_specs = (P("segment", "amp"), P("segment", None))
    return jax.shard_map(body, mesh=mesh, in_specs=in_specs, out_specs=out_specs, check_vma=False)
```

```python
import functools

import jax
import jax.numpy as jnp
from jax import lax
from jax.experimental import pallas as pl
from jax.experimental.pallas import tpu as pltpu
from jax.sharding import PartitionSpec as P

KEEP_FACTORS = (1.0, 0.9, 1.0, 0.97)
FLIP_FACTORS = (0.9, 1.0, 0.97, 1.0)
QUBITS = 7
REG = 128
MID = 16
PEERS = 64
SECTIONS = 4
BLOCKS = 3
ROWS = 2048
MESH = pl.DeviceIdType.MESH
F32 = jnp.float32
BF16 = jnp.bfloat16


def split(x):
    hi = x.astype(BF16)
    lo = (x - hi.astype(F32)).astype(BF16)
    return hi, lo


def exact_dot(a, b):
    return jnp.dot(a, b, precision=lax.Precision.HIGHEST, preferred_element_type=F32)


def mix_rows(gate_cat, x):
    hi, lo = split(x)
    return jnp.dot(gate_cat, jnp.concatenate([hi, hi, lo], axis=0), preferred_element_type=F32)


def mix_lanes(x, gate_cat):
    hi, lo = split(x)
    return jnp.dot(jnp.concatenate([hi, hi, lo], axis=1), gate_cat, preferred_element_type=F32)


def rows_cat(gate):
    hi, lo = split(gate)
    return jnp.concatenate([hi, lo, hi], axis=1)


def lanes_cat(gate_t):
    hi, lo = split(gate_t)
    return jnp.concatenate([hi, lo, hi], axis=0)


def block_transpose(arrays):
    block = lax.broadcasted_iota(jnp.int32, arrays[0].shape, 1) // 16
    for bit in (4, 2, 1):
        low = (block // bit) % 2 == 0
        after = list(arrays)
        for a in range(8):
            if a & bit:
                continue
            here, there = arrays[a], arrays[a + bit]
            if bit == 4:
                moved = pltpu.roll(jnp.where(low, there, here), 64, 1)
                after[a] = jnp.where(low, here, moved)
                after[a + bit] = jnp.where(low, moved, there)
            else:
                after[a] = jnp.where(low, here, pltpu.roll(there, 16 * bit, 1))
                after[a + bit] = jnp.where(low, pltpu.roll(here, REG - 16 * bit, 1), there)
        arrays = after
    return arrays


def fold_squares(acc, x):
    sq = x * x
    return acc + jnp.sum(sq.reshape(sq.shape[0] // 8, 8, sq.shape[1]), axis=0)


def amp_of(m, j):
    return (m // 8) * 32 + (j // 2) * 16 + (m % 8) * 2 + j % 2


def scalar_pick(kind, table):
    return jnp.where(
        kind == 0,
        F32(table[0]),
        jnp.where(kind == 1, F32(table[1]), jnp.where(kind == 2, F32(table[2]), F32(table[3]))),
    )


def kernel(
    states_ref, gate_ref, kraus_hbm, target_hbm,
    y_ref, scale_ref, logs_ref,
    kraus_ref, target_ref, x_ref, all_gates, send1, recv1, mid1, mid2, mid3, quarters, recv2, wide2, send3, recv3, h_mats, l_mats, noises, lows, sums_out, sums_in,
    gate_send, gate_recv, pair_send, pair_recv,
    send1_sem, recv1_sem, send2_sem, recv2_sem, send3_sem, recv3_sem, sums_send, sums_recv,
    load_sems,
):
    seg = lax.axis_index("segment")
    me = lax.axis_index("amp")
    y_me = me // 16
    z_me = (me % 16) // 2
    core = me % 2
    j_me = (y_me % 2) * 2 + core
    m_me = (y_me // 2) * 8 + z_me
    slot_me = m_me * 4 + j_me
    kappa_me = me // 8
    partner = me + 1 - 2 * core
    zero = jnp.zeros((8, REG), F32)

    def part(index, rows):
        return pl.ds(pl.multiple_of(index * rows, rows), rows)

    def wait_bytes(ref, rows, sem):
        pltpu.make_async_copy(ref.at[pl.ds(0, rows)], ref.at[pl.ds(0, rows)], sem).wait()

    loads = [
        pltpu.make_async_copy(states_ref, x_ref, load_sems.at[0]),
        pltpu.make_async_copy(gate_ref.at[0], all_gates.at[seg], load_sems.at[1]),
        pltpu.make_async_copy(kraus_hbm, kraus_ref, load_sems.at[2]),
        pltpu.make_async_copy(target_hbm, target_ref, load_sems.at[3]),
    ]
    for load in loads:
        load.start()

    barrier = pltpu.get_barrier_semaphore()

    def greet(k, carry):
        pl.semaphore_signal(barrier, inc=1, device_id=(seg, (me + k) % PEERS), device_id_type=MESH)
        return carry

    lax.fori_loop(40, PEERS, greet, 0)
    lax.fori_loop(1, 40, greet, 0)
    for k in range(1, SECTIONS):
        pl.semaphore_signal(barrier, inc=1, device_id=((seg + k) % SECTIONS, me), device_id_type=MESH)

    far_first = ((1, 0), (1, 1), (0, 1), (0, 0))
    near_first = far_first[::-1]

    def to_all(send_one, flips=far_first):
        for flip_upper, flip_lower in flips:
            y = ((y_me // 2 + flip_upper) % 2) * 2 + (y_me + flip_lower) % 2
            for on in (1, 0):
                half = (z_me // 4 + on) % 2

                def one(n, carry, y=y, half=half):
                    send_one(y, half * 4 + (z_me + n // 2) % 4, (core + n) % 2)
                    return carry

                lax.fori_loop(0 if flip_upper or flip_lower or on else 1, 8, one, 0)

    width = 16

    def pack(k, acc):
        for i in range(width):
            m = k * width + i
            x = x_ref[pl.ds(m, REG, stride=MID), :]
            acc = fold_squares(acc, x)
            pieces = block_transpose([x[q * 16 : (q + 1) * 16] for q in range(8)])
            for b in range(8):
                send1[part(b % 2 * 64 + m * 4 + b // 2, 16), :] = pieces[b]
        return acc

    loads[0].wait()
    first_sum = lax.fori_loop(0, MID // width, pack, zero)
    for load in loads[1:]:
        load.wait()

    pl.semaphore_wait(barrier, PEERS - 1 + SECTIONS - 1)

    def exchange(e, source, target, piece_of, slot, send_sem, recv_sem, group, flips):
        def one(y, z, c):
            pltpu.make_async_remote_copy(
                source.at[part(e * 64 + piece_of(y, z, c), 16)], target.at[part(e * 64 + slot, 16)],
                send_sem, recv_sem.at[group],
                device_id=(seg, y * 16 + z * 2 + c), device_id_type=MESH,
            ).start()

        to_all(one, flips)

    def piece_by_m(y, z, c):
        return ((y // 2) * 8 + z) * 4 + (y % 2) * 2 + c

    def piece_by_g(y, z, c):
        return y * 16 + z * 2 + c

    my_half = pl.ds(pl.multiple_of(core * 64, 64), 64)
    other_half = pl.ds(pl.multiple_of((1 - core) * 64, 64), 64)

    def gate_copy(section, target_seg):
        return pltpu.make_async_remote_copy(
            all_gates.at[section, :, my_half, :],
            all_gates.at[section, :, my_half, :],
            gate_send.at[target_seg],
            gate_recv.at[section],
            device_id=(target_seg, me),
            device_id_type=MESH,
        )

    def pair_copy(section):
        return pltpu.make_async_remote_copy(
            all_gates.at[section, :, my_half, :],
            all_gates.at[section, :, my_half, :],
            pair_send.at[section],
            pair_recv.at[section],
            device_id=(seg, partner),
            device_id_type=MESH,
        )

    def send_gates(section):
        @pl.when(seg == section)
        def _():
            for k in range(1, SECTIONS):
                gate_copy(section, (seg + k) % SECTIONS).start()

    def pass_gates(section):
        @pl.when(seg != section)
        def _():
            gate_copy(section, section).wait_recv()
            pair_copy(section).start()

    def end_gates(section):
        @pl.when(seg != section)
        def _():
            pltpu.make_async_copy(
                all_gates.at[section, :, other_half, :], all_gates.at[section, :, other_half, :], pair_recv.at[section]
            ).wait()

    row = lax.broadcasted_iota(jnp.int32, (REG, REG), 0)
    col = lax.broadcasted_iota(jnp.int32, (REG, REG), 1)
    identity = (row == col).astype(F32)
    to_split = (col == (row % 64) * 2 + row // 64).astype(F32)
    from_split = (row == (col % 64) * 2 + col // 64).astype(F32)
    to_lanes = (col == (row % 16 // 2) * 16 + (row // 16) * 2 + row % 2).astype(F32)

    def noise(section, block):
        product = jnp.ones((REG, REG), F32)
        for q in range(QUBITS):
            kind = kraus_ref[0, block, section, q]
            bit = lax.shift_right_logical(row, QUBITS - 1 - q) & 1
            product = product * jnp.where(bit == 1, scalar_pick(kind, FLIP_FACTORS), scalar_pick(kind, KEEP_FACTORS))
        return product

    def compose(section):
        low, high = identity, identity
        for block in range(BLOCKS):
            on_low = target_ref[section, block] == 0
            gate = all_gates[section, block]
            if block == 0:
                mixed = gate
            else:
                mixed = exact_dot(gate, jnp.where(on_low, low, high))
            mixed = noises[section, block] * mixed
            low, high = jnp.where(on_low, mixed, low), jnp.where(on_low, high, mixed)
        return low, high

    for section in range(SECTIONS):
        send_gates(section)
    for e in range(2):
        exchange(e, send1, recv1, piece_by_m, me, send1_sem, recv1_sem, e * 8 + kappa_me, far_first)
    for e in range(2):
        recv1[part(e * 64 + me, 16), :] = send1[part(e * 64 + slot_me, 16), :]

    for section in range(SECTIONS):
        for block in range(BLOCKS):
            noises[section, block] = noise(section, block)
    for section in range(SECTIONS):
        pass_gates(section)
    for section in range(SECTIONS):
        end_gates(section)
        low, high = compose(section)
        if section > 0:
            high = exact_dot(high, from_split)
        if section % 2 == 1:
            high = exact_dot(to_lanes if section == 1 else to_split, high)
        h_mats[section] = rows_cat(high)
        lows[section] = low

    def split_rows(ref, index, stride, rows=64):
        return jnp.concatenate(
            [ref[pl.ds(2 * index, rows, stride=stride), :], ref[pl.ds(2 * index + 1, rows, stride=stride), :]], axis=0
        )

    def arrived(ref, sem, group, own, pieces):
        @pl.when(own)
        def _():
            wait_bytes(ref, (pieces - 1) * 16, sem.at[group])

        @pl.when(jnp.logical_not(own))
        def _():
            wait_bytes(ref, pieces * 16, sem.at[group])

    def chunk(wide, i, n):
        return wide[n * 16 : (n + 1) * 16, i * REG : (i + 1) * REG]

    def section0(e):
        def some(steps):
            kappas = []
            for k in steps:
                y = ((y_me // 2 + 1 - k // 2) % 2) * 2 + (y_me + (k + 1) // 2) % 2
                kappas += [y * 2 + (z_me // 4 + on) % 2 for on in (1, 0)]
            tall = []
            for kappa in kappas:
                arrived(recv1, recv1_sem, e * 8 + kappa, kappa == kappa_me, 8)
            for kappa in kappas:
                parts = block_transpose([recv1[part(e * 64 + kappa * 8 + n, 16), :] for n in range(8)])
                tall.append(jnp.concatenate(parts, axis=0))
            wide = mix_rows(h_mats[0], jnp.concatenate(tall, axis=1))
            for i, kappa in enumerate(kappas):
                parts = block_transpose([chunk(wide, i, q) for q in range(8)])
                for n in range(8):
                    mid1[part(e * 64 + kappa * 8 + n, 16), :] = parts[n]

        for steps in ((0, 1, 2, 3),) if e == 0 else ((0, 1), (2, 3)):
            some(steps)

    def half_rows(ref, e):
        return ref.at[pl.ds(e * 1024, 1024)]

    def section1(e):
        source = half_rows(mid1, e)
        wide = mix_rows(h_mats[1], jnp.concatenate([split_rows(source, r, 16) for r in range(8)], axis=1))
        for r in range(8):
            parts = block_transpose([chunk(wide, r, n) for n in range(8)])
            for q in range(8):
                mid2[part(e * 64 + q * 8 + r, 16), :] = parts[q]
                for j in range(4):
                    quarters[pl.ds(((j * 2 + e) * 64 + q * 8 + r) * 4, 4), :] = parts[q][j * 4 : (j + 1) * 4]

    def section2(e):
        source = half_rows(mid2, e)
        wide = mix_rows(h_mats[2], jnp.concatenate([split_rows(source, kappa, 16) for kappa in range(8)], axis=1))
        for kappa in range(8):
            parts = block_transpose([chunk(wide, kappa, q) for q in range(8)])
            for n in range(8):
                mid3[part(e * 64 + kappa * 8 + n, 16), :] = parts[n]

    def section3(e):
        source = half_rows(mid3, e)
        wide = mix_rows(h_mats[3], jnp.concatenate([split_rows(source, r, 16) for r in range(8)], axis=1))
        target = half_rows(send3, e)
        for r in range(8):
            here = wide[:, r * REG : (r + 1) * REG]
            target[pl.ds(2 * r, 64, stride=16), :] = here[:64]
            target[pl.ds(2 * r + 1, 64, stride=16), :] = here[64:]

    def send_quarters(e):
        def one(k, carry):
            j = (j_me + k) % 4
            pltpu.make_async_remote_copy(
                quarters.at[part(j * 2 + e, 256)], recv2.at[part(j_me * 2 + e, 256)], send2_sem, recv2_sem,
                device_id=(seg, (m_me // 8) * 32 + (j // 2) * 16 + z_me * 2 + j % 2), device_id_type=MESH,
            ).start()
            return carry

        lax.fori_loop(1, 4, one, 0)

    for e in range(2):
        section0(e)
        section1(e)
        section2(e)
        send_quarters(e)
        section3(e)
        exchange(e, send3, recv3, piece_by_g, slot_me, send3_sem, recv3_sem, e * 16 + m_me, near_first)
        recv3[part(e * 64 + slot_me, 16), :] = send3[part(e * 64 + me, 16), :]

    low_all = lows[0]
    l_mats[0] = lanes_cat(low_all.T)
    for section in range(1, SECTIONS):
        low_all = exact_dot(lows[section], low_all)
        l_mats[section] = lanes_cat(low_all.T)

    step = 4

    def norm0(k, acc):
        xs = [x_ref[pl.ds(k * step + i, REG, stride=MID), :] for i in range(step)]
        wide = mix_rows(h_mats[0], jnp.concatenate(xs, axis=1))
        tall = jnp.concatenate([wide[:, i * REG : (i + 1) * REG] for i in range(step)], axis=0)
        return fold_squares(acc, mix_lanes(tall, l_mats[0]))

    sum0 = lax.fori_loop(0, MID // step, norm0, zero)
    wait_bytes(recv2, 3 * 512, recv2_sem)
    recv2[part(j_me, 512), :] = quarters[part(j_me, 512), :]

    def norm1(k, acc):
        parts = block_transpose([recv2[pl.ds(pl.multiple_of(b * 256 + k * 64, 64), 64), :] for b in range(8)])
        for n in range(8):
            wide2[pl.ds(pl.multiple_of(n * 256 + k * 64, 64), 64), :] = parts[n]
        return fold_squares(acc, mix_lanes(jnp.concatenate(parts, axis=0), l_mats[1]))

    sum1 = lax.fori_loop(0, 4, norm1, zero)

    def norm2(k, acc):
        xs = [split_rows(wide2.at[part(2 * k + i // 2, 256)], i % 2, 4) for i in range(4)]
        wide = mix_rows(h_mats[2], jnp.concatenate(xs, axis=1))
        tall = jnp.concatenate([wide[:, i * REG : (i + 1) * REG] for i in range(4)], axis=0)
        return fold_squares(acc, mix_lanes(tall, l_mats[2]))

    sum2 = lax.fori_loop(0, 4, norm2, zero)

    def last(k, acc):
        upper = (y_me // 2 + k // 4) % 2
        z = ((z_me // 4 + 1 - k % 4 // 2) % 2) * 4 + 2 * (k % 2)
        ms = [upper * 8 + z, upper * 8 + z + 1]
        tall = []
        for m in ms:
            for e in range(2):
                arrived(recv3, recv3_sem, e * 16 + m, m == m_me, 4)
            tall += block_transpose([recv3[part(b % 2 * 64 + m * 4 + b // 2, 16), :] for b in range(8)])
        mixed = mix_lanes(jnp.concatenate(tall, axis=0), l_mats[3])
        for i, m in enumerate(ms):
            y_ref[pl.ds(m, REG, stride=MID), :] = mixed[i * REG : (i + 1) * REG]
        return fold_squares(acc, mixed)

    sum3 = lax.fori_loop(0, 8, last, zero)

    lane = lax.broadcasted_iota(jnp.int32, (1, REG), 1)
    line = jnp.ones((1, REG), F32)
    for n, acc in enumerate((first_sum, sum0, sum1, sum2, sum3)):
        line = jnp.where(lane == n, jnp.sum(acc), line)
    sums_out[...] = line
    sums_in[me] = line

    def send_sums(y, z, c):
        pltpu.make_async_remote_copy(
            sums_out, sums_in.at[me], sums_send, sums_recv, device_id=(seg, y * 16 + z * 2 + c), device_id_type=MESH
        ).start()

    to_all(send_sums)

    for section in range(SECTIONS):
        @pl.when(seg == section)
        def _():
            for k in range(1, SECTIONS):
                gate_copy(section, (seg + k) % SECTIONS).wait_send()

        @pl.when(seg != section)
        def _():
            pair_copy(section).wait_send()

    wait_bytes(send1, 126 * 16, send1_sem)
    wait_bytes(recv2, 3 * 512, send2_sem)
    wait_bytes(send3, 126 * 16, send3_sem)
    wait_bytes(sums_in, 63, sums_send)
    wait_bytes(sums_in, 63, sums_recv)
    totals = jnp.sum(sums_in[...], axis=0)
    logs_ref[...] = jnp.log(pltpu.roll(totals, REG - 1, 1) / totals)
    mean = jnp.sum(jnp.where(lane == 4, totals, 0.0)) / (PEERS * ROWS * REG)
    scale_ref[...] = 1.0 / jnp.sqrt(jnp.full((1, REG), mean, F32))


def scale_kernel(values_ref, scale_ref, logs_ref, y_ref, log_weights_ref, scaled, logs, sems):
    logs[...] = logs_ref[:, :SECTIONS]
    rows = ROWS // 4
    copies = [pltpu.make_async_copy(logs, log_weights_ref, sems.at[4])]
    for n in range(4):
        part = pl.ds(n * rows, rows)
        scaled[part, :] = values_ref[part, :] * scale_ref[...]
        copies.append(pltpu.make_async_copy(scaled.at[part], y_ref.at[part], sems.at[n]))
        copies[-1].start()
    copies[0].start()
    for copy in copies:
        copy.wait()


def body(states, gate_blocks, kraus_picks, block_targets):
    dma = pltpu.SemaphoreType.DMA
    vmem = pl.BlockSpec(memory_space=pltpu.VMEM)
    anywhere = pl.BlockSpec(memory_space=pl.ANY)
    big = pltpu.VMEM((ROWS, REG), F32)
    line = pltpu.VMEM((1, REG), F32)
    values, scale, logs = pl.pallas_call(
        kernel,
        out_shape=(big, line, line),
        in_specs=[anywhere] * 4,
        out_specs=(vmem, vmem, vmem),
        scratch_shapes=[
            pltpu.SMEM((1, BLOCKS, SECTIONS, QUBITS), jnp.int32),
            pltpu.SMEM((SECTIONS, BLOCKS), jnp.int32),
            big,
            pltpu.VMEM((SECTIONS, BLOCKS, REG, REG), F32),
            big, big, big, big, big, big, big, big, big, big,
            pltpu.VMEM((SECTIONS, REG, 3 * REG), BF16),
            pltpu.VMEM((SECTIONS, 3 * REG, REG), BF16),
            pltpu.VMEM((SECTIONS, BLOCKS, REG, REG), F32),
            pltpu.VMEM((SECTIONS, REG, REG), F32),
            pltpu.VMEM((1, REG), F32),
            pltpu.VMEM((PEERS, 1, REG), F32),
            dma((SECTIONS,)), dma((SECTIONS,)), dma((SECTIONS,)), dma((SECTIONS,)),
            dma, dma((16,)), dma, dma, dma, dma((32,)), dma, dma,
            dma((4,)),
        ],
        compiler_params=pltpu.CompilerParams(collective_id=0, has_side_effects=True),
        name="trajectory",
    )(states.reshape(ROWS, REG), gate_blocks, kraus_picks.transpose(0, 2, 1, 3), block_targets)
    final, log_weights = pl.pallas_call(
        scale_kernel,
        out_shape=(jax.ShapeDtypeStruct((ROWS, REG), F32), jax.ShapeDtypeStruct((1, SECTIONS), F32)),
        in_specs=[vmem, vmem, vmem],
        out_specs=(anywhere, anywhere),
        scratch_shapes=[big, pltpu.VMEM((1, SECTIONS), F32), dma((5,))],
        compiler_params=pltpu.CompilerParams(vmem_limit_bytes=8 * 2**20),
        name="scale",
    )(values, scale, logs)
    return final.reshape(states.shape), log_weights


def solution(mesh):
    in_specs = (
        P("segment", "amp"),
        P("segment", None, None, None),
        P("segment", None, None, None),
        P(),
    )
    out_specs = (P("segment", "amp"), P("segment", None))
    return jax.shard_map(body, mesh=mesh, in_specs=in_specs, out_specs=out_specs, check_vma=False)
```

```python
import functools

import jax
import jax.numpy as jnp
from jax import lax
from jax.experimental import pallas as pl
from jax.experimental.pallas import tpu as pltpu
from jax.sharding import PartitionSpec as P

KEEP_FACTORS = (1.0, 0.9, 1.0, 0.97)
FLIP_FACTORS = (0.9, 1.0, 0.97, 1.0)
QUBITS = 7
REG = 128
MID = 16
PEERS = 64
SECTIONS = 4
BLOCKS = 3
ROWS = 2048
MESH = pl.DeviceIdType.MESH
F32 = jnp.float32
BF16 = jnp.bfloat16


def split(x):
    hi = x.astype(BF16)
    lo = (x - hi.astype(F32)).astype(BF16)
    return hi, lo


def exact_dot(a, b):
    return jnp.dot(a, b, precision=lax.Precision.HIGHEST, preferred_element_type=F32)


def mix_rows(gate_cat, x):
    hi, lo = split(x)
    return jnp.dot(gate_cat, jnp.concatenate([hi, hi, lo], axis=0), preferred_element_type=F32)


def mix_lanes(x, gate_cat):
    hi, lo = split(x)
    return jnp.dot(jnp.concatenate([hi, hi, lo], axis=1), gate_cat, preferred_element_type=F32)


def rows_cat(gate):
    hi, lo = split(gate)
    return jnp.concatenate([hi, lo, hi], axis=1)


def lanes_cat(gate_t):
    hi, lo = split(gate_t)
    return jnp.concatenate([hi, lo, hi], axis=0)


def block_transpose(arrays):
    block = lax.broadcasted_iota(jnp.int32, arrays[0].shape, 1) // 16
    for bit in (4, 2, 1):
        low = (block // bit) % 2 == 0
        after = list(arrays)
        for a in range(8):
            if a & bit:
                continue
            here, there = arrays[a], arrays[a + bit]
            if bit == 4:
                moved = pltpu.roll(jnp.where(low, there, here), 64, 1)
                after[a] = jnp.where(low, here, moved)
                after[a + bit] = jnp.where(low, moved, there)
            else:
                after[a] = jnp.where(low, here, pltpu.roll(there, 16 * bit, 1))
                after[a + bit] = jnp.where(low, pltpu.roll(here, REG - 16 * bit, 1), there)
        arrays = after
    return arrays


def fold_squares(acc, x):
    sq = x * x
    return acc + jnp.sum(sq.reshape(sq.shape[0] // 8, 8, sq.shape[1]), axis=0)


def amp_of(m, j):
    return (m // 8) * 32 + (j // 2) * 16 + (m % 8) * 2 + j % 2


def scalar_pick(kind, table):
    return jnp.where(
        kind == 0,
        F32(table[0]),
        jnp.where(kind == 1, F32(table[1]), jnp.where(kind == 2, F32(table[2]), F32(table[3]))),
    )


def kernel(
    states_ref, gate_ref, kraus_hbm, target_hbm,
    y_ref, scale_ref, logs_ref,
    kraus_ref, target_ref, x_ref, all_gates, send1, recv1, mid1, mid2, mid3, quarters, recv2, wide2, send3, recv3, h_mats, l_mats, noises, lows, sums_out, sums_in,
    gate_send, gate_recv, pair_send, pair_recv,
    send1_sem, recv1_sem, send2_sem, recv2_sem, send3_sem, recv3_sem, sums_send, sums_recv,
    load_sems,
):
    seg = lax.axis_index("segment")
    me = lax.axis_index("amp")
    y_me = me // 16
    z_me = (me % 16) // 2
    core = me % 2
    j_me = (y_me % 2) * 2 + core
    m_me = (y_me // 2) * 8 + z_me
    slot_me = m_me * 4 + j_me
    kappa_me = me // 8
    partner = me + 1 - 2 * core
    zero = jnp.zeros((8, REG), F32)

    def part(index, rows):
        return pl.ds(pl.multiple_of(index * rows, rows), rows)

    def wait_bytes(ref, rows, sem):
        pltpu.make_async_copy(ref.at[pl.ds(0, rows)], ref.at[pl.ds(0, rows)], sem).wait()

    loads = [
        pltpu.make_async_copy(states_ref, x_ref, load_sems.at[0]),
        pltpu.make_async_copy(gate_ref.at[0], all_gates.at[seg], load_sems.at[1]),
        pltpu.make_async_copy(kraus_hbm, kraus_ref, load_sems.at[2]),
        pltpu.make_async_copy(target_hbm, target_ref, load_sems.at[3]),
    ]
    for load in loads:
        load.start()

    barrier = pltpu.get_barrier_semaphore()

    def greet(k, carry):
        pl.semaphore_signal(barrier, inc=1, device_id=(seg, (me + k) % PEERS), device_id_type=MESH)
        return carry

    lax.fori_loop(40, PEERS, greet, 0)
    lax.fori_loop(1, 40, greet, 0)
    for k in range(1, SECTIONS):
        pl.semaphore_signal(barrier, inc=1, device_id=((seg + k) % SECTIONS, me), device_id_type=MESH)

    y_far_first = ((1, 0, 1), (1, 0, 0), (1, 1, 1), (1, 1, 0), (0, 1, 1), (0, 1, 0), (0, 0, 1), (0, 0, 0))
    y_near_first = ((0, 0, 1), (0, 0, 0), (0, 1, 1), (0, 1, 0), (1, 1, 1), (1, 1, 0), (1, 0, 1), (1, 0, 0))
    last_order = ((0, 1), (0, 0), (1, 1), (1, 0))

    def to_all(send_one, flips=y_far_first):
        for flip in flips:
            y = ((y_me // 2 + flip[0]) % 2) * 2 + (y_me + flip[1]) % 2
            half = (z_me // 4 + flip[2]) % 2

            def one(n, carry, y=y, half=half):
                send_one(y, half * 4 + (z_me + n // 2) % 4, (core + n) % 2)
                return carry

            lax.fori_loop(0 if any(flip) else 1, 8, one, 0)

    width = 16

    def pack(k, acc):
        for i in range(width):
            m = k * width + i
            x = x_ref[pl.ds(m, REG, stride=MID), :]
            acc = fold_squares(acc, x)
            pieces = block_transpose([x[q * 16 : (q + 1) * 16] for q in range(8)])
            for b in range(8):
                send1[part(b % 2 * 64 + m * 4 + b // 2, 16), :] = pieces[b]
        return acc

    loads[0].wait()
    first_sum = lax.fori_loop(0, MID // width, pack, zero)
    for load in loads[1:]:
        load.wait()

    pl.semaphore_wait(barrier, PEERS - 1 + SECTIONS - 1)

    def exchange(e, source, target, piece_of, slot, send_sem, recv_sem, group, flips):
        def one(y, z, c):
            pltpu.make_async_remote_copy(
                source.at[part(e * 64 + piece_of(y, z, c), 16)], target.at[part(e * 64 + slot, 16)],
                send_sem, recv_sem.at[group],
                device_id=(seg, y * 16 + z * 2 + c), device_id_type=MESH,
            ).start()

        to_all(one, flips)

    def piece_by_m(y, z, c):
        return ((y // 2) * 8 + z) * 4 + (y % 2) * 2 + c

    def piece_by_g(y, z, c):
        return y * 16 + z * 2 + c

    my_half = pl.ds(pl.multiple_of(core * 64, 64), 64)
    other_half = pl.ds(pl.multiple_of((1 - core) * 64, 64), 64)

    def gate_copy(section, target_seg):
        return pltpu.make_async_remote_copy(
            all_gates.at[section, :, my_half, :],
            all_gates.at[section, :, my_half, :],
            gate_send.at[target_seg],
            gate_recv.at[section],
            device_id=(target_seg, me),
            device_id_type=MESH,
        )

    def pair_copy(section):
        return pltpu.make_async_remote_copy(
            all_gates.at[section, :, my_half, :],
            all_gates.at[section, :, my_half, :],
            pair_send.at[section],
            pair_recv.at[section],
            device_id=(seg, partner),
            device_id_type=MESH,
        )

    def send_gates(section):
        @pl.when(seg == section)
        def _():
            for k in range(1, SECTIONS):
                gate_copy(section, (seg + k) % SECTIONS).start()

    def pass_gates(section):
        @pl.when(seg != section)
        def _():
            gate_copy(section, section).wait_recv()
            pair_copy(section).start()

    def end_gates(section):
        @pl.when(seg != section)
        def _():
            pltpu.make_async_copy(
                all_gates.at[section, :, other_half, :], all_gates.at[section, :, other_half, :], pair_recv.at[section]
            ).wait()

    row = lax.broadcasted_iota(jnp.int32, (REG, REG), 0)
    col = lax.broadcasted_iota(jnp.int32, (REG, REG), 1)
    identity = (row == col).astype(F32)
    to_split = (col == (row % 64) * 2 + row // 64).astype(F32)
    from_split = (row == (col % 64) * 2 + col // 64).astype(F32)
    to_lanes = (col == (row % 16 // 2) * 16 + (row // 16) * 2 + row % 2).astype(F32)

    def noise(section, block):
        product = jnp.ones((REG, REG), F32)
        for q in range(QUBITS):
            kind = kraus_ref[0, block, section, q]
            bit = lax.shift_right_logical(row, QUBITS - 1 - q) & 1
            product = product * jnp.where(bit == 1, scalar_pick(kind, FLIP_FACTORS), scalar_pick(kind, KEEP_FACTORS))
        return product

    def compose(section):
        low, high = identity, identity
        for block in range(BLOCKS):
            on_low = target_ref[section, block] == 0
            gate = all_gates[section, block]
            if block == 0:
                mixed = gate
            else:
                mixed = exact_dot(gate, jnp.where(on_low, low, high))
            mixed = noises[section, block] * mixed
            low, high = jnp.where(on_low, mixed, low), jnp.where(on_low, high, mixed)
        return low, high

    for section in range(SECTIONS):
        send_gates(section)
    for e in range(2):
        exchange(e, send1, recv1, piece_by_m, me, send1_sem, recv1_sem, e * 8 + kappa_me, y_far_first)
    for e in range(2):
        recv1[part(e * 64 + me, 16), :] = send1[part(e * 64 + slot_me, 16), :]

    for section in range(SECTIONS):
        for block in range(BLOCKS):
            noises[section, block] = noise(section, block)
    for section in range(SECTIONS):
        pass_gates(section)
    for section in range(SECTIONS):
        end_gates(section)
        low, high = compose(section)
        if section > 0:
            high = exact_dot(high, from_split)
        if section % 2 == 1:
            high = exact_dot(to_lanes if section == 1 else to_split, high)
        h_mats[section] = rows_cat(high)
        lows[section] = low

    def split_rows(ref, index, stride, rows=64):
        return jnp.concatenate(
            [ref[pl.ds(2 * index, rows, stride=stride), :], ref[pl.ds(2 * index + 1, rows, stride=stride), :]], axis=0
        )

    def arrived(ref, sem, group, own, pieces):
        @pl.when(own)
        def _():
            wait_bytes(ref, (pieces - 1) * 16, sem.at[group])

        @pl.when(jnp.logical_not(own))
        def _():
            wait_bytes(ref, pieces * 16, sem.at[group])

    def chunk(wide, i, n):
        return wide[n * 16 : (n + 1) * 16, i * REG : (i + 1) * REG]

    def section0(e):
        def some(steps):
            kappas = []
            for k in steps:
                y = ((y_me // 2 + 1 - k // 2) % 2) * 2 + (y_me + (k + 1) // 2) % 2
                kappas += [y * 2 + (z_me // 4 + on) % 2 for on in (1, 0)]
            tall = []
            for kappa in kappas:
                arrived(recv1, recv1_sem, e * 8 + kappa, kappa == kappa_me, 8)
            for kappa in kappas:
                parts = block_transpose([recv1[part(e * 64 + kappa * 8 + n, 16), :] for n in range(8)])
                tall.append(jnp.concatenate(parts, axis=0))
            wide = mix_rows(h_mats[0], jnp.concatenate(tall, axis=1))
            for i, kappa in enumerate(kappas):
                parts = block_transpose([chunk(wide, i, q) for q in range(8)])
                for n in range(8):
                    mid1[part(e * 64 + kappa * 8 + n, 16), :] = parts[n]

        for steps in ((0, 1, 2, 3),) if e == 0 else ((0, 1), (2, 3)):
            some(steps)

    def half_rows(ref, e):
        return ref.at[pl.ds(e * 1024, 1024)]

    def section1(e):
        source = half_rows(mid1, e)
        wide = mix_rows(h_mats[1], jnp.concatenate([split_rows(source, r, 16) for r in range(8)], axis=1))
        for r in range(8):
            parts = block_transpose([chunk(wide, r, n) for n in range(8)])
            for q in range(8):
                mid2[part(e * 64 + q * 8 + r, 16), :] = parts[q]
                for j in range(4):
                    quarters[pl.ds(((j * 2 + e) * 64 + q * 8 + r) * 4, 4), :] = parts[q][j * 4 : (j + 1) * 4]

    def section2(e):
        source = half_rows(mid2, e)
        wide = mix_rows(h_mats[2], jnp.concatenate([split_rows(source, kappa, 16) for kappa in range(8)], axis=1))
        for kappa in range(8):
            parts = block_transpose([chunk(wide, kappa, q) for q in range(8)])
            for n in range(8):
                mid3[part(e * 64 + kappa * 8 + n, 16), :] = parts[n]

    def section3(e):
        source = half_rows(mid3, e)
        wide = mix_rows(h_mats[3], jnp.concatenate([split_rows(source, r, 16) for r in range(8)], axis=1))
        target = half_rows(send3, e)
        for r in range(8):
            here = wide[:, r * REG : (r + 1) * REG]
            target[pl.ds(2 * r, 64, stride=16), :] = here[:64]
            target[pl.ds(2 * r + 1, 64, stride=16), :] = here[64:]

    def send_quarters(e):
        def one(k, carry):
            j = (j_me + k) % 4
            pltpu.make_async_remote_copy(
                quarters.at[part(j * 2 + e, 256)], recv2.at[part(j_me * 2 + e, 256)], send2_sem, recv2_sem,
                device_id=(seg, (m_me // 8) * 32 + (j // 2) * 16 + z_me * 2 + j % 2), device_id_type=MESH,
            ).start()
            return carry

        lax.fori_loop(1, 4, one, 0)

    for e in range(2):
        section0(e)
        section1(e)
        section2(e)
        send_quarters(e)
        section3(e)
        exchange(e, send3, recv3, piece_by_g, slot_me, send3_sem, recv3_sem, e * 16 + m_me, y_near_first)
        recv3[part(e * 64 + slot_me, 16), :] = send3[part(e * 64 + me, 16), :]

    low_all = lows[0]
    l_mats[0] = lanes_cat(low_all.T)
    for section in range(1, SECTIONS):
        low_all = exact_dot(lows[section], low_all)
        l_mats[section] = lanes_cat(low_all.T)

    step = 4

    def norm0(k, acc):
        xs = [x_ref[pl.ds(k * step + i, REG, stride=MID), :] for i in range(step)]
        wide = mix_rows(h_mats[0], jnp.concatenate(xs, axis=1))
        tall = jnp.concatenate([wide[:, i * REG : (i + 1) * REG] for i in range(step)], axis=0)
        return fold_squares(acc, mix_lanes(tall, l_mats[0]))

    sum0 = lax.fori_loop(0, MID // step, norm0, zero)
    wait_bytes(recv2, 3 * 512, recv2_sem)
    recv2[part(j_me, 512), :] = quarters[part(j_me, 512), :]

    def norm1(k, acc):
        parts = block_transpose([recv2[pl.ds(pl.multiple_of(b * 256 + k * 64, 64), 64), :] for b in range(8)])
        for n in range(8):
            wide2[pl.ds(pl.multiple_of(n * 256 + k * 64, 64), 64), :] = parts[n]
        return fold_squares(acc, mix_lanes(jnp.concatenate(parts, axis=0), l_mats[1]))

    sum1 = lax.fori_loop(0, 4, norm1, zero)

    def norm2(k, acc):
        xs = [split_rows(wide2.at[part(2 * k + i // 2, 256)], i % 2, 4) for i in range(4)]
        wide = mix_rows(h_mats[2], jnp.concatenate(xs, axis=1))
        tall = jnp.concatenate([wide[:, i * REG : (i + 1) * REG] for i in range(4)], axis=0)
        return fold_squares(acc, mix_lanes(tall, l_mats[2]))

    sum2 = lax.fori_loop(0, 4, norm2, zero)

    def last(upper, half, count, k, acc):
        ms = [upper * 8 + half * 4 + k * count + i for i in range(count)]
        tall = []
        for m in ms:
            for e in range(2):
                arrived(recv3, recv3_sem, e * 16 + m, m == m_me, 4)
            tall += block_transpose([recv3[part(b % 2 * 64 + m * 4 + b // 2, 16), :] for b in range(8)])
        mixed = mix_lanes(jnp.concatenate(tall, axis=0), l_mats[3])
        for i, m in enumerate(ms):
            y_ref[pl.ds(m, REG, stride=MID), :] = mixed[i * REG : (i + 1) * REG]
        return fold_squares(acc, mixed)

    sum3 = zero
    for flip_upper, flip_half in last_order:
        upper = (y_me // 2 + flip_upper) % 2
        half = (z_me // 4 + flip_half) % 2
        count = 1 if (flip_upper, flip_half) == last_order[-1] else 2
        sum3 = lax.fori_loop(0, 4 // count, functools.partial(last, upper, half, count), sum3)

    lane = lax.broadcasted_iota(jnp.int32, (1, REG), 1)
    line = jnp.ones((1, REG), F32)
    for n, acc in enumerate((first_sum, sum0, sum1, sum2, sum3)):
        line = jnp.where(lane == n, jnp.sum(acc), line)
    sums_out[...] = line
    sums_in[me] = line

    def send_sums(y, z, c):
        pltpu.make_async_remote_copy(
            sums_out, sums_in.at[me], sums_send, sums_recv, device_id=(seg, y * 16 + z * 2 + c), device_id_type=MESH
        ).start()

    to_all(send_sums)

    for section in range(SECTIONS):
        @pl.when(seg == section)
        def _():
            for k in range(1, SECTIONS):
                gate_copy(section, (seg + k) % SECTIONS).wait_send()

        @pl.when(seg != section)
        def _():
            pair_copy(section).wait_send()

    wait_bytes(send1, 126 * 16, send1_sem)
    wait_bytes(recv2, 3 * 512, send2_sem)
    wait_bytes(send3, 126 * 16, send3_sem)
    wait_bytes(sums_in, 63, sums_send)
    wait_bytes(sums_in, 63, sums_recv)
    totals = jnp.sum(sums_in[...], axis=0)
    logs_ref[...] = jnp.log(pltpu.roll(totals, REG - 1, 1) / totals)
    mean = jnp.sum(jnp.where(lane == 4, totals, 0.0)) / (PEERS * ROWS * REG)
    scale_ref[...] = 1.0 / jnp.sqrt(jnp.full((1, REG), mean, F32))


def scale_kernel(values_ref, scale_ref, logs_ref, y_ref, log_weights_ref, scaled, logs, sems):
    logs[...] = logs_ref[:, :SECTIONS]
    rows = ROWS // 4
    copies = [pltpu.make_async_copy(logs, log_weights_ref, sems.at[4])]
    for n in range(4):
        part = pl.ds(n * rows, rows)
        scaled[part, :] = values_ref[part, :] * scale_ref[...]
        copies.append(pltpu.make_async_copy(scaled.at[part], y_ref.at[part], sems.at[n]))
        copies[-1].start()
    copies[0].start()
    for copy in copies:
        copy.wait()


def body(states, gate_blocks, kraus_picks, block_targets):
    dma = pltpu.SemaphoreType.DMA
    vmem = pl.BlockSpec(memory_space=pltpu.VMEM)
    anywhere = pl.BlockSpec(memory_space=pl.ANY)
    big = pltpu.VMEM((ROWS, REG), F32)
    line = pltpu.VMEM((1, REG), F32)
    values, scale, logs = pl.pallas_call(
        kernel,
        out_shape=(big, line, line),
        in_specs=[anywhere] * 4,
        out_specs=(vmem, vmem, vmem),
        scratch_shapes=[
            pltpu.SMEM((1, BLOCKS, SECTIONS, QUBITS), jnp.int32),
            pltpu.SMEM((SECTIONS, BLOCKS), jnp.int32),
            big,
            pltpu.VMEM((SECTIONS, BLOCKS, REG, REG), F32),
            big, big, big, big, big, big, big, big, big, big,
            pltpu.VMEM((SECTIONS, REG, 3 * REG), BF16),
            pltpu.VMEM((SECTIONS, 3 * REG, REG), BF16),
            pltpu.VMEM((SECTIONS, BLOCKS, REG, REG), F32),
            pltpu.VMEM((SECTIONS, REG, REG), F32),
            pltpu.VMEM((1, REG), F32),
            pltpu.VMEM((PEERS, 1, REG), F32),
            dma((SECTIONS,)), dma((SECTIONS,)), dma((SECTIONS,)), dma((SECTIONS,)),
            dma, dma((16,)), dma, dma, dma, dma((32,)), dma, dma,
            dma((4,)),
        ],
        compiler_params=pltpu.CompilerParams(collective_id=0, has_side_effects=True),
        name="trajectory",
    )(states.reshape(ROWS, REG), gate_blocks, kraus_picks.transpose(0, 2, 1, 3), block_targets)
    final, log_weights = pl.pallas_call(
        scale_kernel,
        out_shape=(jax.ShapeDtypeStruct((ROWS, REG), F32), jax.ShapeDtypeStruct((1, SECTIONS), F32)),
        in_specs=[vmem, vmem, vmem],
        out_specs=(anywhere, anywhere),
        scratch_shapes=[big, pltpu.VMEM((1, SECTIONS), F32), dma((5,))],
        compiler_params=pltpu.CompilerParams(vmem_limit_bytes=8 * 2**20),
        name="scale",
    )(values, scale, logs)
    return final.reshape(states.shape), log_weights


def solution(mesh):
    in_specs = (
        P("segment", "amp"),
        P("segment", None, None, None),
        P("segment", None, None, None),
        P(),
    )
    out_specs = (P("segment", "amp"), P("segment", None))
    return jax.shard_map(body, mesh=mesh, in_specs=in_specs, out_specs=out_specs, check_vma=False)
```

```python
import functools

import jax
import jax.numpy as jnp
from jax import lax
from jax.experimental import pallas as pl
from jax.experimental.pallas import tpu as pltpu
from jax.sharding import PartitionSpec as P

KEEP_FACTORS = (1.0, 0.9, 1.0, 0.97)
FLIP_FACTORS = (0.9, 1.0, 0.97, 1.0)
QUBITS = 7
REG = 128
MID = 16
PEERS = 64
SECTIONS = 4
BLOCKS = 3
ROWS = 2048
MESH = pl.DeviceIdType.MESH
F32 = jnp.float32
BF16 = jnp.bfloat16


def split(x):
    hi = x.astype(BF16)
    lo = (x - hi.astype(F32)).astype(BF16)
    return hi, lo


def exact_dot(a, b):
    return jnp.dot(a, b, precision=lax.Precision.HIGHEST, preferred_element_type=F32)


def mix_rows(gate_cat, x):
    hi, lo = split(x)
    return jnp.dot(gate_cat, jnp.concatenate([hi, hi, lo], axis=0), preferred_element_type=F32)


def mix_lanes(x, gate_cat):
    hi, lo = split(x)
    return jnp.dot(jnp.concatenate([hi, hi, lo], axis=1), gate_cat, preferred_element_type=F32)


def rows_cat(gate):
    hi, lo = split(gate)
    return jnp.concatenate([hi, lo, hi], axis=1)


def lanes_cat(gate_t):
    hi, lo = split(gate_t)
    return jnp.concatenate([hi, lo, hi], axis=0)


def block_transpose(arrays):
    block = lax.broadcasted_iota(jnp.int32, arrays[0].shape, 1) // 16
    for bit in (4, 2, 1):
        low = (block // bit) % 2 == 0
        after = list(arrays)
        for a in range(8):
            if a & bit:
                continue
            here, there = arrays[a], arrays[a + bit]
            if bit == 4:
                moved = pltpu.roll(jnp.where(low, there, here), 64, 1)
                after[a] = jnp.where(low, here, moved)
                after[a + bit] = jnp.where(low, moved, there)
            else:
                after[a] = jnp.where(low, here, pltpu.roll(there, 16 * bit, 1))
                after[a + bit] = jnp.where(low, pltpu.roll(here, REG - 16 * bit, 1), there)
        arrays = after
    return arrays


def fold_squares(acc, x):
    sq = x * x
    return acc + jnp.sum(sq.reshape(sq.shape[0] // 8, 8, sq.shape[1]), axis=0)


def amp_of(m, j):
    return (m // 8) * 32 + (j // 2) * 16 + (m % 8) * 2 + j % 2


def scalar_pick(kind, table):
    return jnp.where(
        kind == 0,
        F32(table[0]),
        jnp.where(kind == 1, F32(table[1]), jnp.where(kind == 2, F32(table[2]), F32(table[3]))),
    )


def kernel(
    states_ref, gate_ref, kraus_hbm, target_hbm,
    y_ref, scale_ref, logs_ref,
    kraus_ref, target_ref, x_ref, all_gates, send1, recv1, mid1, mid2, mid3, quarters, recv2, wide2, send3, recv3, h_mats, l_mats, noises, lows, sums_out, sums_in,
    gate_send, gate_recv, pair_send, pair_recv,
    send1_sem, recv1_sem, send2_sem, recv2_sem, send3_sem, recv3_sem, sums_send, sums_recv,
    load_sems,
):
    seg = lax.axis_index("segment")
    me = lax.axis_index("amp")
    y_me = me // 16
    z_me = (me % 16) // 2
    core = me % 2
    j_me = (y_me % 2) * 2 + core
    m_me = (y_me // 2) * 8 + z_me
    slot_me = m_me * 4 + j_me
    kappa_me = me // 8
    partner = me + 1 - 2 * core
    zero = jnp.zeros((8, REG), F32)

    def part(index, rows):
        return pl.ds(pl.multiple_of(index * rows, rows), rows)

    def wait_bytes(ref, rows, sem):
        pltpu.make_async_copy(ref.at[pl.ds(0, rows)], ref.at[pl.ds(0, rows)], sem).wait()

    loads = [
        pltpu.make_async_copy(states_ref, x_ref, load_sems.at[0]),
        pltpu.make_async_copy(gate_ref.at[0], all_gates.at[seg], load_sems.at[1]),
        pltpu.make_async_copy(kraus_hbm, kraus_ref, load_sems.at[2]),
        pltpu.make_async_copy(target_hbm, target_ref, load_sems.at[3]),
    ]
    for load in loads:
        load.start()

    barrier = pltpu.get_barrier_semaphore()

    def greet(k, carry):
        pl.semaphore_signal(barrier, inc=1, device_id=(seg, (me + k) % PEERS), device_id_type=MESH)
        return carry

    lax.fori_loop(34, PEERS, greet, 0)
    lax.fori_loop(1, 34, greet, 0)
    for k in range(1, SECTIONS):
        pl.semaphore_signal(barrier, inc=1, device_id=((seg + k) % SECTIONS, me), device_id_type=MESH)

    far_first = ((1, 0), (1, 1), (0, 1), (0, 0))
    near_first = far_first[::-1]

    def to_all(send_one, flips=far_first):
        for flip_upper, flip_lower in flips:
            y = ((y_me // 2 + flip_upper) % 2) * 2 + (y_me + flip_lower) % 2
            for on in (1, 0):
                half = (z_me // 4 + on) % 2

                def one(n, carry, y=y, half=half):
                    send_one(y, half * 4 + (z_me + n // 2) % 4, (core + n) % 2)
                    return carry

                lax.fori_loop(0 if flip_upper or flip_lower or on else 1, 8, one, 0)

    width = 16

    def pack(k, acc):
        for i in range(width):
            m = k * width + i
            x = x_ref[pl.ds(m, REG, stride=MID), :]
            acc = fold_squares(acc, x)
            pieces = block_transpose([x[q * 16 : (q + 1) * 16] for q in range(8)])
            for b in range(8):
                send1[part(b % 2 * 64 + m * 4 + b // 2, 16), :] = pieces[b]
        return acc

    loads[0].wait()
    first_sum = lax.fori_loop(0, MID // width, pack, zero)
    for load in loads[1:]:
        load.wait()

    pl.semaphore_wait(barrier, PEERS - 1 + SECTIONS - 1)

    def exchange(e, source, target, piece_of, slot, send_sem, recv_sem, group, flips):
        def one(y, z, c):
            pltpu.make_async_remote_copy(
                source.at[part(e * 64 + piece_of(y, z, c), 16)], target.at[part(e * 64 + slot, 16)],
                send_sem, recv_sem.at[group],
                device_id=(seg, y * 16 + z * 2 + c), device_id_type=MESH,
            ).start()

        to_all(one, flips)

    def piece_by_m(y, z, c):
        return ((y // 2) * 8 + z) * 4 + (y % 2) * 2 + c

    def piece_by_g(y, z, c):
        return y * 16 + z * 2 + c

    my_half = pl.ds(pl.multiple_of(core * 64, 64), 64)
    other_half = pl.ds(pl.multiple_of((1 - core) * 64, 64), 64)

    def gate_copy(section, target_seg):
        return pltpu.make_async_remote_copy(
            all_gates.at[section, :, my_half, :],
            all_gates.at[section, :, my_half, :],
            gate_send.at[target_seg],
            gate_recv.at[section],
            device_id=(target_seg, me),
            device_id_type=MESH,
        )

    def pair_copy(section):
        return pltpu.make_async_remote_copy(
            all_gates.at[section, :, my_half, :],
            all_gates.at[section, :, my_half, :],
            pair_send.at[section],
            pair_recv.at[section],
            device_id=(seg, partner),
            device_id_type=MESH,
        )

    def send_gates(section):
        @pl.when(seg == section)
        def _():
            for k in range(1, SECTIONS):
                gate_copy(section, (seg + k) % SECTIONS).start()

    def pass_gates(section):
        @pl.when(seg != section)
        def _():
            gate_copy(section, section).wait_recv()
            pair_copy(section).start()

    def end_gates(section):
        @pl.when(seg != section)
        def _():
            pltpu.make_async_copy(
                all_gates.at[section, :, other_half, :], all_gates.at[section, :, other_half, :], pair_recv.at[section]
            ).wait()

    row = lax.broadcasted_iota(jnp.int32, (REG, REG), 0)
    col = lax.broadcasted_iota(jnp.int32, (REG, REG), 1)
    identity = (row == col).astype(F32)
    to_split = (col == (row % 64) * 2 + row // 64).astype(F32)
    from_split = (row == (col % 64) * 2 + col // 64).astype(F32)
    to_lanes = (col == (row % 16 // 2) * 16 + (row // 16) * 2 + row % 2).astype(F32)

    def noise(section, block):
        product = jnp.ones((REG, REG), F32)
        for q in range(QUBITS):
            kind = kraus_ref[0, block, section, q]
            bit = lax.shift_right_logical(row, QUBITS - 1 - q) & 1
            product = product * jnp.where(bit == 1, scalar_pick(kind, FLIP_FACTORS), scalar_pick(kind, KEEP_FACTORS))
        return product

    def compose(section):
        low, high = identity, identity
        for block in range(BLOCKS):
            on_low = target_ref[section, block] == 0
            gate = all_gates[section, block]
            if block == 0:
                mixed = gate
            else:
                mixed = exact_dot(gate, jnp.where(on_low, low, high))
            mixed = noises[section, block] * mixed
            low, high = jnp.where(on_low, mixed, low), jnp.where(on_low, high, mixed)
        return low, high

    for section in range(SECTIONS):
        send_gates(section)
    for e in range(2):
        exchange(e, send1, recv1, piece_by_m, me, send1_sem, recv1_sem, e * 8 + kappa_me, far_first)
    for e in range(2):
        recv1[part(e * 64 + me, 16), :] = send1[part(e * 64 + slot_me, 16), :]

    for section in range(SECTIONS):
        for block in range(BLOCKS):
            noises[section, block] = noise(section, block)
    for section in range(SECTIONS):
        pass_gates(section)
    for section in range(SECTIONS):
        end_gates(section)
        low, high = compose(section)
        if section > 0:
            high = exact_dot(high, from_split)
        if section % 2 == 1:
            high = exact_dot(to_lanes if section == 1 else to_split, high)
        h_mats[section] = rows_cat(high)
        lows[section] = low

    def split_rows(ref, index, stride, rows=64):
        return jnp.concatenate(
            [ref[pl.ds(2 * index, rows, stride=stride), :], ref[pl.ds(2 * index + 1, rows, stride=stride), :]], axis=0
        )

    def arrived(ref, sem, group, own, pieces):
        @pl.when(own)
        def _():
            wait_bytes(ref, (pieces - 1) * 16, sem.at[group])

        @pl.when(jnp.logical_not(own))
        def _():
            wait_bytes(ref, pieces * 16, sem.at[group])

    def chunk(wide, i, n):
        return wide[n * 16 : (n + 1) * 16, i * REG : (i + 1) * REG]

    def section0(e):
        def some(steps):
            kappas = []
            for k in steps:
                y = ((y_me // 2 + 1 - k // 2) % 2) * 2 + (y_me + (k + 1) // 2) % 2
                kappas += [y * 2 + (z_me // 4 + on) % 2 for on in (1, 0)]
            tall = []
            for kappa in kappas:
                arrived(recv1, recv1_sem, e * 8 + kappa, kappa == kappa_me, 8)
            for kappa in kappas:
                parts = block_transpose([recv1[part(e * 64 + kappa * 8 + n, 16), :] for n in range(8)])
                tall.append(jnp.concatenate(parts, axis=0))
            wide = mix_rows(h_mats[0], jnp.concatenate(tall, axis=1))
            for i, kappa in enumerate(kappas):
                parts = block_transpose([chunk(wide, i, q) for q in range(8)])
                for n in range(8):
                    mid1[part(e * 64 + kappa * 8 + n, 16), :] = parts[n]

        for steps in ((0, 1, 2, 3),) if e == 0 else ((0, 1), (2, 3)):
            some(steps)

    def half_rows(ref, e):
        return ref.at[pl.ds(e * 1024, 1024)]

    def section1(e):
        source = half_rows(mid1, e)
        wide = mix_rows(h_mats[1], jnp.concatenate([split_rows(source, r, 16) for r in range(8)], axis=1))
        for r in range(8):
            parts = block_transpose([chunk(wide, r, n) for n in range(8)])
            for q in range(8):
                mid2[part(e * 64 + q * 8 + r, 16), :] = parts[q]
                for j in range(4):
                    quarters[pl.ds(((j * 2 + e) * 64 + q * 8 + r) * 4, 4), :] = parts[q][j * 4 : (j + 1) * 4]

    def section2(e):
        source = half_rows(mid2, e)
        wide = mix_rows(h_mats[2], jnp.concatenate([split_rows(source, kappa, 16) for kappa in range(8)], axis=1))
        for kappa in range(8):
            parts = block_transpose([chunk(wide, kappa, q) for q in range(8)])
            for n in range(8):
                mid3[part(e * 64 + kappa * 8 + n, 16), :] = parts[n]

    def section3(e):
        source = half_rows(mid3, e)
        wide = mix_rows(h_mats[3], jnp.concatenate([split_rows(source, r, 16) for r in range(8)], axis=1))
        target = half_rows(send3, e)
        for r in range(8):
            here = wide[:, r * REG : (r + 1) * REG]
            target[pl.ds(2 * r, 64, stride=16), :] = here[:64]
            target[pl.ds(2 * r + 1, 64, stride=16), :] = here[64:]

    def send_quarters(e):
        def one(k, carry):
            j = (j_me + k) % 4
            pltpu.make_async_remote_copy(
                quarters.at[part(j * 2 + e, 256)], recv2.at[part(j_me * 2 + e, 256)], send2_sem, recv2_sem,
                device_id=(seg, (m_me // 8) * 32 + (j // 2) * 16 + z_me * 2 + j % 2), device_id_type=MESH,
            ).start()
            return carry

        lax.fori_loop(1, 4, one, 0)

    for e in range(2):
        section0(e)
        section1(e)
        section2(e)
        send_quarters(e)
        section3(e)
        exchange(e, send3, recv3, piece_by_g, slot_me, send3_sem, recv3_sem, e * 16 + m_me, near_first)
        recv3[part(e * 64 + slot_me, 16), :] = send3[part(e * 64 + me, 16), :]

    low_all = lows[0]
    l_mats[0] = lanes_cat(low_all.T)
    for section in range(1, SECTIONS):
        low_all = exact_dot(lows[section], low_all)
        l_mats[section] = lanes_cat(low_all.T)

    step = 4

    def norm0(k, acc):
        xs = [x_ref[pl.ds(k * step + i, REG, stride=MID), :] for i in range(step)]
        wide = mix_rows(h_mats[0], jnp.concatenate(xs, axis=1))
        tall = jnp.concatenate([wide[:, i * REG : (i + 1) * REG] for i in range(step)], axis=0)
        return fold_squares(acc, mix_lanes(tall, l_mats[0]))

    sum0 = lax.fori_loop(0, MID // step, norm0, zero)
    wait_bytes(recv2, 3 * 512, recv2_sem)
    recv2[part(j_me, 512), :] = quarters[part(j_me, 512), :]

    def norm1(k, acc):
        parts = block_transpose([recv2[pl.ds(pl.multiple_of(b * 256 + k * 64, 64), 64), :] for b in range(8)])
        for n in range(8):
            wide2[pl.ds(pl.multiple_of(n * 256 + k * 64, 64), 64), :] = parts[n]
        return fold_squares(acc, mix_lanes(jnp.concatenate(parts, axis=0), l_mats[1]))

    sum1 = lax.fori_loop(0, 4, norm1, zero)

    def norm2(k, acc):
        xs = [split_rows(wide2.at[part(2 * k + i // 2, 256)], i % 2, 4) for i in range(4)]
        wide = mix_rows(h_mats[2], jnp.concatenate(xs, axis=1))
        tall = jnp.concatenate([wide[:, i * REG : (i + 1) * REG] for i in range(4)], axis=0)
        return fold_squares(acc, mix_lanes(tall, l_mats[2]))

    sum2 = lax.fori_loop(0, 4, norm2, zero)

    for section in range(SECTIONS):
        @pl.when(seg == section)
        def _():
            for k in range(1, SECTIONS):
                gate_copy(section, (seg + k) % SECTIONS).wait_send()

        @pl.when(seg != section)
        def _():
            pair_copy(section).wait_send()

    wait_bytes(send1, 126 * 16, send1_sem)
    wait_bytes(recv2, 3 * 512, send2_sem)

    lane = lax.broadcasted_iota(jnp.int32, (1, REG), 1)
    known = jnp.ones((1, REG), F32)
    for n, acc in enumerate((first_sum, sum0, sum1, sum2)):
        known = jnp.where(lane == n, jnp.sum(acc), known)
    sums_out[...] = known

    def last(k, acc):
        upper = (y_me // 2 + k // 4) % 2
        z = ((z_me // 4 + 1 - k % 4 // 2) % 2) * 4 + 2 * (k % 2)
        ms = [upper * 8 + z, upper * 8 + z + 1]
        tall = []
        for m in ms:
            for e in range(2):
                arrived(recv3, recv3_sem, e * 16 + m, m == m_me, 4)
            tall += block_transpose([recv3[part(b % 2 * 64 + m * 4 + b // 2, 16), :] for b in range(8)])
        mixed = mix_lanes(jnp.concatenate(tall, axis=0), l_mats[3])
        for i, m in enumerate(ms):
            y_ref[pl.ds(m, REG, stride=MID), :] = mixed[i * REG : (i + 1) * REG]
        return fold_squares(acc, mixed)

    sum3 = lax.fori_loop(0, 8, last, zero)

    line = jnp.where(lane == 4, jnp.sum(sum3), sums_out[...])
    sums_out[...] = line
    sums_in[me] = line

    def send_sums(y, z, c):
        pltpu.make_async_remote_copy(
            sums_out, sums_in.at[me], sums_send, sums_recv, device_id=(seg, y * 16 + z * 2 + c), device_id_type=MESH
        ).start()

    to_all(send_sums)

    wait_bytes(send3, 126 * 16, send3_sem)
    wait_bytes(sums_in, 63, sums_send)
    wait_bytes(sums_in, 63, sums_recv)
    totals = jnp.sum(sums_in[...], axis=0)
    logs_ref[...] = jnp.log(pltpu.roll(totals, REG - 1, 1) / totals)
    mean = jnp.sum(jnp.where(lane == 4, totals, 0.0)) / (PEERS * ROWS * REG)
    scale_ref[...] = 1.0 / jnp.sqrt(jnp.full((1, REG), mean, F32))


def scale_kernel(values_ref, scale_ref, logs_ref, y_ref, log_weights_ref, scaled, logs, sems):
    logs[...] = logs_ref[:, :SECTIONS]
    rows = ROWS // 4
    copies = [pltpu.make_async_copy(logs, log_weights_ref, sems.at[4])]
    for n in range(4):
        part = pl.ds(n * rows, rows)
        scaled[part, :] = values_ref[part, :] * scale_ref[...]
        copies.append(pltpu.make_async_copy(scaled.at[part], y_ref.at[part], sems.at[n]))
        copies[-1].start()
    copies[0].start()
    for copy in copies:
        copy.wait()


def body(states, gate_blocks, kraus_picks, block_targets):
    dma = pltpu.SemaphoreType.DMA
    vmem = pl.BlockSpec(memory_space=pltpu.VMEM)
    anywhere = pl.BlockSpec(memory_space=pl.ANY)
    big = pltpu.VMEM((ROWS, REG), F32)
    line = pltpu.VMEM((1, REG), F32)
    values, scale, logs = pl.pallas_call(
        kernel,
        out_shape=(big, line, line),
        in_specs=[anywhere] * 4,
        out_specs=(vmem, vmem, vmem),
        scratch_shapes=[
            pltpu.SMEM((1, BLOCKS, SECTIONS, QUBITS), jnp.int32),
            pltpu.SMEM((SECTIONS, BLOCKS), jnp.int32),
            big,
            pltpu.VMEM((SECTIONS, BLOCKS, REG, REG), F32),
            big, big, big, big, big, big, big, big, big, big,
            pltpu.VMEM((SECTIONS, REG, 3 * REG), BF16),
            pltpu.VMEM((SECTIONS, 3 * REG, REG), BF16),
            pltpu.VMEM((SECTIONS, BLOCKS, REG, REG), F32),
            pltpu.VMEM((SECTIONS, REG, REG), F32),
            pltpu.VMEM((1, REG), F32),
            pltpu.VMEM((PEERS, 1, REG), F32),
            dma((SECTIONS,)), dma((SECTIONS,)), dma((SECTIONS,)), dma((SECTIONS,)),
            dma, dma((16,)), dma, dma, dma, dma((32,)), dma, dma,
            dma((4,)),
        ],
        compiler_params=pltpu.CompilerParams(collective_id=0, has_side_effects=True),
        name="trajectory",
    )(states.reshape(ROWS, REG), gate_blocks, kraus_picks.transpose(0, 2, 1, 3), block_targets)
    final, log_weights = pl.pallas_call(
        scale_kernel,
        out_shape=(jax.ShapeDtypeStruct((ROWS, REG), F32), jax.ShapeDtypeStruct((1, SECTIONS), F32)),
        in_specs=[vmem, vmem, vmem],
        out_specs=(anywhere, anywhere),
        scratch_shapes=[big, pltpu.VMEM((1, SECTIONS), F32), dma((5,))],
        compiler_params=pltpu.CompilerParams(vmem_limit_bytes=8 * 2**20),
        name="scale",
    )(values, scale, logs)
    return final.reshape(states.shape), log_weights


def solution(mesh):
    in_specs = (
        P("segment", "amp"),
        P("segment", None, None, None),
        P("segment", None, None, None),
        P(),
    )
    out_specs = (P("segment", "amp"), P("segment", None))
    return jax.shard_map(body, mesh=mesh, in_specs=in_specs, out_specs=out_specs, check_vma=False)
```

```python
import functools

import jax
import jax.numpy as jnp
from jax import lax
from jax.experimental import pallas as pl
from jax.experimental.pallas import tpu as pltpu
from jax.sharding import PartitionSpec as P

KEEP_FACTORS = (1.0, 0.9, 1.0, 0.97)
FLIP_FACTORS = (0.9, 1.0, 0.97, 1.0)
QUBITS = 7
REG = 128
MID = 16
PEERS = 64
SECTIONS = 4
BLOCKS = 3
ROWS = 2048
MESH = pl.DeviceIdType.MESH
F32 = jnp.float32
BF16 = jnp.bfloat16


def split(x):
    hi = x.astype(BF16)
    lo = (x - hi.astype(F32)).astype(BF16)
    return hi, lo


def exact_dot(a, b):
    return jnp.dot(a, b, precision=lax.Precision.HIGHEST, preferred_element_type=F32)


def mix_rows(gate_cat, x):
    hi, lo = split(x)
    return jnp.dot(gate_cat, jnp.concatenate([hi, hi, lo], axis=0), preferred_element_type=F32)


def mix_lanes(x, gate_cat):
    hi, lo = split(x)
    return jnp.dot(jnp.concatenate([hi, hi, lo], axis=1), gate_cat, preferred_element_type=F32)


def rows_cat(gate):
    hi, lo = split(gate)
    return jnp.concatenate([hi, lo, hi], axis=1)


def lanes_cat(gate_t):
    hi, lo = split(gate_t)
    return jnp.concatenate([hi, lo, hi], axis=0)


def block_transpose(arrays):
    block = lax.broadcasted_iota(jnp.int32, arrays[0].shape, 1) // 16
    for bit in (4, 2, 1):
        low = (block // bit) % 2 == 0
        after = list(arrays)
        for a in range(8):
            if a & bit:
                continue
            here, there = arrays[a], arrays[a + bit]
            if bit == 4:
                moved = pltpu.roll(jnp.where(low, there, here), 64, 1)
                after[a] = jnp.where(low, here, moved)
                after[a + bit] = jnp.where(low, moved, there)
            else:
                after[a] = jnp.where(low, here, pltpu.roll(there, 16 * bit, 1))
                after[a + bit] = jnp.where(low, pltpu.roll(here, REG - 16 * bit, 1), there)
        arrays = after
    return arrays


def fold_squares(acc, x):
    sq = x * x
    return acc + jnp.sum(sq.reshape(sq.shape[0] // 8, 8, sq.shape[1]), axis=0)


def amp_of(m, j):
    return (m // 8) * 32 + (j // 2) * 16 + (m % 8) * 2 + j % 2


def scalar_pick(kind, table):
    return jnp.where(
        kind == 0,
        F32(table[0]),
        jnp.where(kind == 1, F32(table[1]), jnp.where(kind == 2, F32(table[2]), F32(table[3]))),
    )


def kernel(
    states_ref, gate_ref, kraus_hbm, target_hbm,
    y_ref, scale_ref, logs_ref,
    kraus_ref, target_ref, x_ref, all_gates, send1, recv1, mid1, mid2, mid3, quarters, recv2, wide2, send3, recv3, h_mats, l_mats, noises, lows, sums_out, sums_in,
    gate_send, gate_recv, pair_send, pair_recv,
    send1_sem, recv1_sem, send2_sem, recv2_sem, send3_sem, recv3_sem, sums_send, sums_recv,
    load_sems,
):
    seg = lax.axis_index("segment")
    me = lax.axis_index("amp")
    y_me = me // 16
    z_me = (me % 16) // 2
    core = me % 2
    j_me = (y_me % 2) * 2 + core
    m_me = (y_me // 2) * 8 + z_me
    slot_me = m_me * 4 + j_me
    kappa_me = me // 8
    partner = me + 1 - 2 * core
    zero = jnp.zeros((8, REG), F32)

    def part(index, rows):
        return pl.ds(pl.multiple_of(index * rows, rows), rows)

    def wait_bytes(ref, rows, sem):
        pltpu.make_async_copy(ref.at[pl.ds(0, rows)], ref.at[pl.ds(0, rows)], sem).wait()

    loads = [
        pltpu.make_async_copy(states_ref, x_ref, load_sems.at[0]),
        pltpu.make_async_copy(gate_ref.at[0], all_gates.at[seg], load_sems.at[1]),
        pltpu.make_async_copy(kraus_hbm, kraus_ref, load_sems.at[2]),
        pltpu.make_async_copy(target_hbm, target_ref, load_sems.at[3]),
    ]
    for load in loads:
        load.start()

    barrier = pltpu.get_barrier_semaphore()

    def greet(k, carry):
        pl.semaphore_signal(barrier, inc=1, device_id=(seg, (me + k) % PEERS), device_id_type=MESH)
        return carry

    lax.fori_loop(40, PEERS, greet, 0)
    lax.fori_loop(1, 40, greet, 0)
    for k in range(1, SECTIONS):
        pl.semaphore_signal(barrier, inc=1, device_id=((seg + k) % SECTIONS, me), device_id_type=MESH)

    far_first = ((1, 0), (1, 1), (0, 1), (0, 0))
    near_first = far_first[::-1]

    def to_all(send_one, flips=far_first):
        for flip_upper, flip_lower in flips:
            y = ((y_me // 2 + flip_upper) % 2) * 2 + (y_me + flip_lower) % 2
            for on in (1, 0):
                half = (z_me // 4 + on) % 2

                def one(n, carry, y=y, half=half):
                    send_one(y, half * 4 + (z_me + n // 2) % 4, (core + n) % 2)
                    return carry

                lax.fori_loop(0 if flip_upper or flip_lower or on else 1, 8, one, 0)

    width = 16

    def pack(k, acc):
        for i in range(width):
            m = k * width + i
            x = x_ref[pl.ds(m, REG, stride=MID), :]
            acc = fold_squares(acc, x)
            pieces = block_transpose([x[q * 16 : (q + 1) * 16] for q in range(8)])
            for b in range(8):
                send1[part(b % 2 * 64 + m * 4 + b // 2, 16), :] = pieces[b]
        return acc

    loads[0].wait()
    first_sum = lax.fori_loop(0, MID // width, pack, zero)
    for load in loads[1:]:
        load.wait()

    pl.semaphore_wait(barrier, PEERS - 1 + SECTIONS - 1)

    def exchange(e, source, target, piece_of, slot, send_sem, recv_sem, group, flips):
        def one(y, z, c):
            pltpu.make_async_remote_copy(
                source.at[part(e * 64 + piece_of(y, z, c), 16)], target.at[part(e * 64 + slot, 16)],
                send_sem, recv_sem.at[group],
                device_id=(seg, y * 16 + z * 2 + c), device_id_type=MESH,
            ).start()

        to_all(one, flips)

    def piece_by_m(y, z, c):
        return ((y // 2) * 8 + z) * 4 + (y % 2) * 2 + c

    def piece_by_g(y, z, c):
        return y * 16 + z * 2 + c

    my_half = pl.ds(pl.multiple_of(core * 64, 64), 64)
    other_half = pl.ds(pl.multiple_of((1 - core) * 64, 64), 64)

    def gate_copy(section, target_seg):
        return pltpu.make_async_remote_copy(
            all_gates.at[section, :, my_half, :],
            all_gates.at[section, :, my_half, :],
            gate_send.at[target_seg],
            gate_recv.at[section],
            device_id=(target_seg, me),
            device_id_type=MESH,
        )

    def pair_copy(section):
        return pltpu.make_async_remote_copy(
            all_gates.at[section, :, my_half, :],
            all_gates.at[section, :, my_half, :],
            pair_send.at[section],
            pair_recv.at[section],
            device_id=(seg, partner),
            device_id_type=MESH,
        )

    def send_gates(section):
        @pl.when(seg == section)
        def _():
            for k in range(1, SECTIONS):
                gate_copy(section, (seg + k) % SECTIONS).start()

    def pass_gates(section):
        @pl.when(seg != section)
        def _():
            gate_copy(section, section).wait_recv()
            pair_copy(section).start()

    def end_gates(section):
        @pl.when(seg != section)
        def _():
            pltpu.make_async_copy(
                all_gates.at[section, :, other_half, :], all_gates.at[section, :, other_half, :], pair_recv.at[section]
            ).wait()

    row = lax.broadcasted_iota(jnp.int32, (REG, REG), 0)
    col = lax.broadcasted_iota(jnp.int32, (REG, REG), 1)
    identity = (row == col).astype(F32)
    to_split = (col == (row % 64) * 2 + row // 64).astype(F32)
    from_split = (row == (col % 64) * 2 + col // 64).astype(F32)
    to_lanes = (col == (row % 16 // 2) * 16 + (row // 16) * 2 + row % 2).astype(F32)

    def noise(section, block):
        product = jnp.ones((REG, REG), F32)
        for q in range(QUBITS):
            kind = kraus_ref[0, block, section, q]
            bit = lax.shift_right_logical(row, QUBITS - 1 - q) & 1
            product = product * jnp.where(bit == 1, scalar_pick(kind, FLIP_FACTORS), scalar_pick(kind, KEEP_FACTORS))
        return product

    def compose(section):
        low, high = identity, identity
        for block in range(BLOCKS):
            on_low = target_ref[section, block] == 0
            gate = all_gates[section, block]
            if block == 0:
                mixed = gate
            else:
                mixed = exact_dot(gate, jnp.where(on_low, low, high))
            mixed = noises[section, block] * mixed
            low, high = jnp.where(on_low, mixed, low), jnp.where(on_low, high, mixed)
        return low, high

    for section in range(SECTIONS):
        send_gates(section)
    for e in range(2):
        exchange(e, send1, recv1, piece_by_m, me, send1_sem, recv1_sem, e * 8 + kappa_me, far_first)
    for e in range(2):
        recv1[part(e * 64 + me, 16), :] = send1[part(e * 64 + slot_me, 16), :]

    for section in range(SECTIONS):
        for block in range(BLOCKS):
            noises[section, block] = noise(section, block)
    for section in range(SECTIONS):
        pass_gates(section)
    for section in range(SECTIONS):
        end_gates(section)
        low, high = compose(section)
        if section > 0:
            high = exact_dot(high, from_split)
        if section % 2 == 1:
            high = exact_dot(to_lanes if section == 1 else to_split, high)
        h_mats[section] = rows_cat(high)
        lows[section] = low

    def split_rows(ref, index, stride, rows=64):
        return jnp.concatenate(
            [ref[pl.ds(2 * index, rows, stride=stride), :], ref[pl.ds(2 * index + 1, rows, stride=stride), :]], axis=0
        )

    def arrived(ref, sem, group, own, pieces):
        @pl.when(own)
        def _():
            wait_bytes(ref, (pieces - 1) * 16, sem.at[group])

        @pl.when(jnp.logical_not(own))
        def _():
            wait_bytes(ref, pieces * 16, sem.at[group])

    def chunk(wide, i, n):
        return wide[n * 16 : (n + 1) * 16, i * REG : (i + 1) * REG]

    def section0(e):
        def some(steps):
            kappas = []
            for k in steps:
                y = ((y_me // 2 + 1 - k // 2) % 2) * 2 + (y_me + (k + 1) // 2) % 2
                kappas += [y * 2 + (z_me // 4 + on) % 2 for on in (1, 0)]
            tall = []
            for kappa in kappas:
                arrived(recv1, recv1_sem, e * 8 + kappa, kappa == kappa_me, 8)
            for kappa in kappas:
                parts = block_transpose([recv1[part(e * 64 + kappa * 8 + n, 16), :] for n in range(8)])
                tall.append(jnp.concatenate(parts, axis=0))
            wide = mix_rows(h_mats[0], jnp.concatenate(tall, axis=1))
            for i, kappa in enumerate(kappas):
                parts = block_transpose([chunk(wide, i, q) for q in range(8)])
                for n in range(8):
                    mid1[part(e * 64 + kappa * 8 + n, 16), :] = parts[n]

        for steps in ((0, 1, 2, 3),) if e == 0 else ((0, 1), (2, 3)):
            some(steps)

    def half_rows(ref, e):
        return ref.at[pl.ds(e * 1024, 1024)]

    def section1(e):
        source = half_rows(mid1, e)
        wide = mix_rows(h_mats[1], jnp.concatenate([split_rows(source, r, 16) for r in range(8)], axis=1))
        for r in range(8):
            parts = block_transpose([chunk(wide, r, n) for n in range(8)])
            for q in range(8):
                mid2[part(e * 64 + q * 8 + r, 16), :] = parts[q]
                for j in range(4):
                    quarters[pl.ds(((j * 2 + e) * 64 + q * 8 + r) * 4, 4), :] = parts[q][j * 4 : (j + 1) * 4]

    def section2(e):
        source = half_rows(mid2, e)
        wide = mix_rows(h_mats[2], jnp.concatenate([split_rows(source, kappa, 16) for kappa in range(8)], axis=1))
        for kappa in range(8):
            parts = block_transpose([chunk(wide, kappa, q) for q in range(8)])
            for n in range(8):
                mid3[part(e * 64 + kappa * 8 + n, 16), :] = parts[n]

    def section3(e):
        source = half_rows(mid3, e)
        wide = mix_rows(h_mats[3], jnp.concatenate([split_rows(source, r, 16) for r in range(8)], axis=1))
        target = half_rows(send3, e)
        for r in range(8):
            here = wide[:, r * REG : (r + 1) * REG]
            target[pl.ds(2 * r, 64, stride=16), :] = here[:64]
            target[pl.ds(2 * r + 1, 64, stride=16), :] = here[64:]

    def send_quarters(e):
        def one(k, carry):
            j = (j_me + k) % 4
            pltpu.make_async_remote_copy(
                quarters.at[part(j * 2 + e, 256)], recv2.at[part(j_me * 2 + e, 256)], send2_sem, recv2_sem,
                device_id=(seg, (m_me // 8) * 32 + (j // 2) * 16 + z_me * 2 + j % 2), device_id_type=MESH,
            ).start()
            return carry

        lax.fori_loop(1, 4, one, 0)

    for e in range(2):
        section0(e)
        section1(e)
        section2(e)
        send_quarters(e)
        section3(e)
        exchange(e, send3, recv3, piece_by_g, slot_me, send3_sem, recv3_sem, e * 16 + m_me, near_first)
        recv3[part(e * 64 + slot_me, 16), :] = send3[part(e * 64 + me, 16), :]

    low_all = lows[0]
    l_mats[0] = lanes_cat(low_all.T)
    for section in range(1, SECTIONS):
        low_all = exact_dot(lows[section], low_all)
        l_mats[section] = lanes_cat(low_all.T)

    step = 4

    def norm0(k, acc):
        xs = [x_ref[pl.ds(k * step + i, REG, stride=MID), :] for i in range(step)]
        wide = mix_rows(h_mats[0], jnp.concatenate(xs, axis=1))
        tall = jnp.concatenate([wide[:, i * REG : (i + 1) * REG] for i in range(step)], axis=0)
        return fold_squares(acc, mix_lanes(tall, l_mats[0]))

    sum0 = lax.fori_loop(0, MID // step, norm0, zero)
    wait_bytes(recv2, 3 * 512, recv2_sem)
    recv2[part(j_me, 512), :] = quarters[part(j_me, 512), :]

    def norm1(k, acc):
        parts = block_transpose([recv2[pl.ds(pl.multiple_of(b * 256 + k * 64, 64), 64), :] for b in range(8)])
        for n in range(8):
            wide2[pl.ds(pl.multiple_of(n * 256 + k * 64, 64), 64), :] = parts[n]
        return fold_squares(acc, mix_lanes(jnp.concatenate(parts, axis=0), l_mats[1]))

    sum1 = lax.fori_loop(0, 4, norm1, zero)

    def norm2(k, acc):
        xs = [split_rows(wide2.at[part(2 * k + i // 2, 256)], i % 2, 4) for i in range(4)]
        wide = mix_rows(h_mats[2], jnp.concatenate(xs, axis=1))
        tall = jnp.concatenate([wide[:, i * REG : (i + 1) * REG] for i in range(4)], axis=0)
        return fold_squares(acc, mix_lanes(tall, l_mats[2]))

    sum2 = lax.fori_loop(0, 4, norm2, zero)

    def last(k, acc):
        upper = (y_me // 2 + k // 4) % 2
        z = ((z_me // 4 + 1 - k % 4 // 2) % 2) * 4 + 2 * (k % 2)
        ms = [upper * 8 + z, upper * 8 + z + 1]
        tall = []
        for m in ms:
            for e in range(2):
                arrived(recv3, recv3_sem, e * 16 + m, m == m_me, 4)
            tall += block_transpose([recv3[part(b % 2 * 64 + m * 4 + b // 2, 16), :] for b in range(8)])
        mixed = mix_lanes(jnp.concatenate(tall, axis=0), l_mats[3])
        for i, m in enumerate(ms):
            y_ref[pl.ds(m, REG, stride=MID), :] = mixed[i * REG : (i + 1) * REG]
        return fold_squares(acc, mixed)

    sum3 = lax.fori_loop(0, 8, last, zero)

    lane = lax.broadcasted_iota(jnp.int32, (1, REG), 1)
    line = jnp.ones((1, REG), F32)
    for n, acc in enumerate((first_sum, sum0, sum1, sum2, sum3)):
        line = jnp.where(lane == n, jnp.sum(acc), line)
    sums_out[...] = line
    sums_in[me] = line

    def send_sums(y, z, c):
        pltpu.make_async_remote_copy(
            sums_out, sums_in.at[me], sums_send, sums_recv, device_id=(seg, y * 16 + z * 2 + c), device_id_type=MESH
        ).start()

    to_all(send_sums)

    for section in range(SECTIONS):
        @pl.when(seg == section)
        def _():
            for k in range(1, SECTIONS):
                gate_copy(section, (seg + k) % SECTIONS).wait_send()

        @pl.when(seg != section)
        def _():
            pair_copy(section).wait_send()

    wait_bytes(send1, 126 * 16, send1_sem)
    wait_bytes(recv2, 3 * 512, send2_sem)
    wait_bytes(send3, 126 * 16, send3_sem)
    wait_bytes(sums_in, 63, sums_send)
    wait_bytes(sums_in, 63, sums_recv)
    totals = jnp.sum(sums_in[...], axis=0)
    logs_ref[...] = jnp.log(pltpu.roll(totals, REG - 1, 1) / totals)
    mean = jnp.sum(jnp.where(lane == 4, totals, 0.0)) / (PEERS * ROWS * REG)
    scale_ref[...] = 1.0 / jnp.sqrt(jnp.full((1, REG), mean, F32))


def scale_kernel(values_ref, scale_ref, logs_ref, y_ref, log_weights_ref, scaled, logs, sems):
    logs[...] = logs_ref[:, :SECTIONS]
    rows = ROWS // 8
    copies = [pltpu.make_async_copy(logs, log_weights_ref, sems.at[8])]
    for n in range(8):
        part = pl.ds(n * rows, rows)
        scaled[part, :] = values_ref[part, :] * scale_ref[...]
        copies.append(pltpu.make_async_copy(scaled.at[part], y_ref.at[part], sems.at[n]))
        copies[-1].start()
    copies[0].start()
    for copy in copies:
        copy.wait()


def body(states, gate_blocks, kraus_picks, block_targets):
    dma = pltpu.SemaphoreType.DMA
    vmem = pl.BlockSpec(memory_space=pltpu.VMEM)
    anywhere = pl.BlockSpec(memory_space=pl.ANY)
    big = pltpu.VMEM((ROWS, REG), F32)
    line = pltpu.VMEM((1, REG), F32)
    values, scale, logs = pl.pallas_call(
        kernel,
        out_shape=(big, line, line),
        in_specs=[anywhere] * 4,
        out_specs=(vmem, vmem, vmem),
        scratch_shapes=[
            pltpu.SMEM((1, BLOCKS, SECTIONS, QUBITS), jnp.int32),
            pltpu.SMEM((SECTIONS, BLOCKS), jnp.int32),
            big,
            pltpu.VMEM((SECTIONS, BLOCKS, REG, REG), F32),
            big, big, big, big, big, big, big, big, big, big,
            pltpu.VMEM((SECTIONS, REG, 3 * REG), BF16),
            pltpu.VMEM((SECTIONS, 3 * REG, REG), BF16),
            pltpu.VMEM((SECTIONS, BLOCKS, REG, REG), F32),
            pltpu.VMEM((SECTIONS, REG, REG), F32),
            pltpu.VMEM((1, REG), F32),
            pltpu.VMEM((PEERS, 1, REG), F32),
            dma((SECTIONS,)), dma((SECTIONS,)), dma((SECTIONS,)), dma((SECTIONS,)),
            dma, dma((16,)), dma, dma, dma, dma((32,)), dma, dma,
            dma((4,)),
        ],
        compiler_params=pltpu.CompilerParams(collective_id=0, has_side_effects=True),
        name="trajectory",
    )(states.reshape(ROWS, REG), gate_blocks, kraus_picks.transpose(0, 2, 1, 3), block_targets)
    final, log_weights = pl.pallas_call(
        scale_kernel,
        out_shape=(jax.ShapeDtypeStruct((ROWS, REG), F32), jax.ShapeDtypeStruct((1, SECTIONS), F32)),
        in_specs=[vmem, vmem, vmem],
        out_specs=(anywhere, anywhere),
        scratch_shapes=[big, pltpu.VMEM((1, SECTIONS), F32), dma((9,))],
        compiler_params=pltpu.CompilerParams(vmem_limit_bytes=8 * 2**20),
        name="scale",
    )(values, scale, logs)
    return final.reshape(states.shape), log_weights


def solution(mesh):
    in_specs = (
        P("segment", "amp"),
        P("segment", None, None, None),
        P("segment", None, None, None),
        P(),
    )
    out_specs = (P("segment", "amp"), P("segment", None))
    return jax.shard_map(body, mesh=mesh, in_specs=in_specs, out_specs=out_specs, check_vma=False)
```
